512 devices in a mesh: tile: 128 (over y, z, core), lev: 4 (over x).
Axes of the slice: x: 4, y: 4, z: 16, core: 2. Of those that a mesh axis runs over, the one named last changes fastest.
Arguments:
- trajectory: bfloat16 [3, 32, 262144], P(None, 'lev', 'tile'), may hold values from -6 to 6
- increment: bfloat16 [3, 32, 262144], P(None, 'lev', 'tile'), may hold values from -6 to 6
- counts: int32 [128, 8], P('tile'), may hold values from 1 to 512, 2048 in all within a row
- remap_weight: bfloat16 [128, 8, 512, 512], P('tile'), may hold values from -0.25 to 0.25
- kappa: float32 [3], replicated, may hold values from 0.1 to 0.4
- courant: float32 [262144], P('tile'), may hold values from 0.1 to 0.6
- vertical: float32 [262144], P('tile'), may hold values from -0.4 to 0.4
- offset: int32 [262144], P('tile'), may hold values from -2 to 2
Outputs:
- tangent: float32 [3, 32, 262144], P(None, 'lev', 'tile')
- grad_outer: float32 [3, 32, 262144], P(None, 'lev', 'tile')
The draws below stay inside these ranges and needn't reach their ends.
Inputs may be any that keep to these rules, and one draw needn't show every extreme that they name: Each row of counts sums to 2048, and every row has an entry equal to 512.
All inputs are finite; a program needn't handle non-finite values.
Results may differ from the reference program's by a relative error of at most 0.0021.
The reference program's roundings to bfloat16 on the way count: a program that leaves them out, or rounds other values in their place, can miss the bound.
Values may be sent and summed in bfloat16 or wider, within the bound.
A program may use at most 64 MiB of HBM per device.

```python
import math
import jax
import jax.numpy as jnp
import numpy as np
from jax import lax

TRACERS = 3
LEVELS = 32
REACH = 8
OC_DEV = 2048
HALO = 2
OCOLS = 262144
ICOLS = 262144
CAP = 512
SPAN = 256
WIN = 512
N_TILE = 128


def plant(result, stream_key, smallest, largest):
    spot = [jax.random.randint(jax.random.fold_in(stream_key, axis), (), 0, length) for axis, length in enumerate(result.shape)]
    longest = result.shape.index(max(result.shape))
    neighbour = spot[:longest] + [(spot[longest] + 1) % result.shape[longest]] + spot[longest + 1:]
    return result.at[tuple(spot)].set(smallest).at[tuple(neighbour)].set(largest)


def level_of(stream_key, dims, cuts, low, high):
    def one(dim, parts):
        steps = jax.random.uniform(jax.random.fold_in(jax.random.fold_in(stream_key, 6), dim), (parts,), jnp.float32, low / len(cuts), high / len(cuts))
        return jnp.repeat(jnp.exp(steps), dims[dim] // parts).reshape((-1,) + (1,) * (len(dims) - dim - 1))

    gain = one(*cuts[0])
    for cut in cuts[1:]:
        gain = gain * one(*cut)
    return gain


def split_up(amount, total, limit, skew):
    loads = [(1 << 20) // math.isqrt(rank ** skew) + 1 for rank in range(2, amount + 1)]
    spare, holding = total - limit - (amount - 1), [1] * (amount - 1)
    while spare > 0:
        free = [i for i in range(amount - 1) if holding[i] < limit]
        whole, budget = sum([loads[i] for i in free]), spare
        for i in free:
            addition = min(limit - holding[i], max(1, budget * loads[i] // whole), spare)
            holding[i] = holding[i] + addition
            spare = spare - addition
    return np.array([limit] + holding)


def ragged_sizes(stream_key, amount, total, reach, lean):
    if amount == 2:
        one = jax.random.randint(stream_key, (), max(1, total - reach), min(reach, total - 1) + 1)
        return jnp.stack([one, total - one])
    sizes = jnp.asarray(split_up(amount, total, reach, lean), jnp.int32)
    couples = (amount - 1) // 2
    donor, taker = sizes[1:1 + 2 * couples:2], sizes[2:2 + 2 * couples:2]
    slack = jnp.minimum(donor - 1, reach - taker)
    shifted = jax.random.randint(jax.random.fold_in(stream_key, 1), (couples,), 0, 1 << 20) % (slack + 1)
    sizes = sizes.at[1:1 + 2 * couples:2].set(donor - shifted).at[2:2 + 2 * couples:2].set(taker + shifted)
    return sizes[jax.random.permutation(jax.random.fold_in(stream_key, 2), amount)]


def gaussian(stream_key, shape, spread, bound, shards=(), kind=jnp.bfloat16):
    entries = spread * jax.random.normal(stream_key, shape, jnp.float32)
    if shards:
        entries = entries * level_of(stream_key, shape, shards, -0.22, 0.18)
    return jnp.clip(entries, -bound, bound).astype(kind)


def setup_inputs(seed: int = 0) -> dict:
    seeds = jax.random.split(jax.random.key(seed), 9)
    return {
        "trajectory": gaussian(seeds[0], (TRACERS, LEVELS, OCOLS), 1.0, 6.0, ((1, 4), (2, 128))),
        "increment": gaussian(seeds[1], (TRACERS, LEVELS, OCOLS), 1.0, 6.0, ((1, 4), (2, 128))),
        "counts": jax.vmap(lambda own: ragged_sizes(own, REACH, OC_DEV, CAP, 2))(jax.random.split(seeds[2], N_TILE)).reshape((N_TILE, REACH)).astype(jnp.int32),
        "remap_weight": gaussian(seeds[3], (N_TILE, REACH, WIN, CAP), CAP ** -0.5, 0.25, ((0, 128),)),
        "kappa": jnp.clip(jnp.exp(jax.random.uniform(seeds[4], (TRACERS,), jnp.float32, math.log(0.1), math.log(0.4))), 0.1, 0.4),
        "courant": jnp.clip(0.1 + 0.5 * jax.random.uniform(seeds[5], (ICOLS,), jnp.float32) ** level_of(seeds[5], (ICOLS,), ((0, 128),), -0.2, 0.2), 0.1, 0.6),
        "vertical": jnp.clip(jax.random.uniform(seeds[6], (ICOLS,), jnp.float32, -0.4, 0.4) * level_of(seeds[6], (ICOLS,), ((0, 128),), -0.4, 0.0), -0.4, 0.4),
        "offset": plant(jax.random.randint(seeds[7], (ICOLS,), -HALO, HALO + 1), jax.random.fold_in(seeds[7], 1), -HALO, HALO).astype(jnp.int32),
    }


highest = lax.Precision.HIGHEST


def column_slots(sizes_row, slot_count, column_count):
    sizes_row = sizes_row.astype(jnp.int32)
    group_end = jnp.cumsum(sizes_row).astype(jnp.int32)
    group_start = (group_end - sizes_row).astype(jnp.int32)
    position = jnp.arange(slot_count, dtype=jnp.int32)
    slot_index = jnp.minimum(group_start[:, None] + position[None, :], column_count - 1).astype(jnp.int32)
    slot_live = position[None, :] < sizes_row[:, None]
    columns = jnp.arange(column_count, dtype=jnp.int32)
    owner = jnp.searchsorted(group_end, columns, side="right").astype(jnp.int32)
    back_index = (owner * slot_count + columns - jnp.take(group_start, owner)).astype(jnp.int32)
    return slot_index, slot_live, back_index


def shifted_levels(field, upward):
    zero_level = jnp.zeros_like(field[:, :1])
    if upward:
        return jnp.concatenate([field[:, 1:], zero_level], axis=1)
    return jnp.concatenate([zero_level, field[:, :-1]], axis=1)


def reference(trajectory, increment, counts, remap_weight, kappa, courant, vertical, offset):
    field_rows = TRACERS * LEVELS
    centre = REACH // 2
    fields = jnp.concatenate([trajectory, increment], axis=0).reshape(2 * field_rows, OCOLS)
    senders = jnp.arange(N_TILE, dtype=jnp.int32)
    reach_ids = jnp.arange(REACH, dtype=jnp.int32)

    def forward_sender(sender):
        slot_index, slot_live, back_index = column_slots(counts[sender], CAP, OC_DEV)
        own_cols = lax.dynamic_slice_in_dim(fields, (sender * OC_DEV).astype(jnp.int32), OC_DEV, 1)
        slotted = jnp.take(own_cols, slot_index.reshape(-1), axis=1).reshape(2 * field_rows, REACH, CAP)
        slotted = jnp.where(slot_live[None], slotted, jnp.zeros_like(slotted))
        return jnp.einsum("fdc,dwc->dfw", slotted.astype(jnp.float32), remap_weight[sender].astype(jnp.float32), precision=highest)

    partial_value = lax.map(forward_sender, senders)
    source = ((senders[:, None] - reach_ids[None, :] + centre) % N_TILE).astype(jnp.int32)
    received = partial_value[source, reach_ids[None, :]]
    blocks = received[:, :, :, :SPAN] + jnp.roll(received[:, :, :, SPAN:], 1, axis=1)
    remapped = jnp.transpose(blocks, (2, 0, 1, 3)).reshape(2 * field_rows, ICOLS)
    state = remapped[:field_rows].reshape(TRACERS, LEVELS, ICOLS)
    delta = remapped[field_rows:].reshape(TRACERS, LEVELS, ICOLS)

    rising = jnp.maximum(vertical, 0.0)
    sinking = jnp.maximum(-vertical, 0.0)
    departed = jnp.zeros_like(delta)
    for shift_by in range(-HALO, HALO + 1):
        moved_view = jnp.roll(delta, -shift_by, axis=2)
        departed = departed + jnp.where(offset == shift_by, moved_view, jnp.zeros_like(moved_view))
    below = shifted_levels(delta, False)
    above = shifted_levels(delta, True)
    loss = 2.0 * kappa[:, None, None] * state
    tangent = delta + courant * (departed - delta) + rising * (below - delta) + sinking * (above - delta) - loss * delta

    arrived = jnp.zeros_like(tangent)
    for shift_by in range(-HALO, HALO + 1):
        weight_row = jnp.where(offset == shift_by, courant, jnp.zeros_like(courant))
        arrived = arrived + jnp.roll(weight_row * tangent, shift_by, axis=2)
    diagonal = 1.0 - courant - rising - sinking - loss
    adjoint = diagonal * tangent + arrived + rising * shifted_levels(tangent, True) + sinking * shifted_levels(tangent, False)

    adjoint_blocks = jnp.transpose(adjoint.reshape(field_rows, N_TILE, REACH, SPAN), (1, 2, 0, 3)).astype(jnp.bfloat16)
    windows = jnp.concatenate([adjoint_blocks, jnp.roll(adjoint_blocks, -1, axis=1)], axis=3)
    target = ((senders[:, None] + reach_ids[None, :] - centre) % N_TILE).astype(jnp.int32)
    returned_all = windows[target, reach_ids[None, :]]

    def backward_sender(sender):
        slot_index, slot_live, back_index = column_slots(counts[sender], CAP, OC_DEV)
        slot_grad = jnp.einsum("dfw,dwc->fdc", returned_all[sender].astype(jnp.float32), remap_weight[sender].astype(jnp.float32), precision=highest)
        return jnp.take(slot_grad.reshape(field_rows, REACH * CAP), back_index, axis=1)

    grads = lax.map(backward_sender, senders)
    grad_outer = jnp.transpose(grads, (1, 0, 2)).reshape(TRACERS, LEVELS, OCOLS)
    return tangent, grad_outer
```

```python
import functools

import jax
import jax.numpy as jnp
from jax import lax
from jax.experimental import pallas as pl
from jax.experimental.pallas import tpu as pltpu
from jax.sharding import PartitionSpec as P

MESH = pl.DeviceIdType.MESH
LANES = 128
HALO = 2
SEND_ORDER = (0, 7, 1, 6, 2, 5, 3, 4)


def kernel(
    n_tile,
    n_lev,
    traj_ref,
    inc_ref,
    counts_ref,
    kappa_ref,
    courant_ref,
    vertical_ref,
    offset_ref,
    weight_hbm,
    tangent_out,
    grad_out,
    weight,
    shifted,
    fields,
    outgoing,
    recv,
    coef,
    delta,
    loss,
    tang,
    up_out,
    down_out,
    below_in,
    above_in,
    adj,
    back,
    placed,
    weight_sem,
    fwd_send,
    fwd_recv,
    coef_send,
    coef_recv,
    col_send,
    col_recv,
    lev_send,
    lev_recv,
    ret_send,
    ret_recv,
):
    tracers, levels, cols = traj_ref.shape
    rows = tracers * levels
    reach = weight_hbm.shape[1]
    win, cap = weight_hbm.shape[2], weight_hbm.shape[3]
    centre = reach // 2
    span = cols // reach
    tiles = cols // LANES
    sub = span // LANES
    me = lax.axis_index("tile")
    lev = lax.axis_index("lev")

    def tile_at(distance):
        return (lax.rem(me + (n_tile + distance), n_tile), lev)

    weight_copies = [
        pltpu.make_async_copy(weight_hbm.at[0, d], weight.at[d], weight_sem.at[d]) for d in range(reach)
    ]
    for d in SEND_ORDER:
        weight_copies[d].start()

    barrier = pltpu.get_barrier_semaphore()
    for distance in range(-centre, centre + 1):
        if distance != 0:
            pl.semaphore_signal(barrier, inc=1, device_id=tile_at(distance), device_id_type=MESH)

    @pl.when(lev > 0)
    def _():
        pl.semaphore_signal(barrier, inc=1, device_id=(me, lev - 1), device_id_type=MESH)

    @pl.when(lev < n_lev - 1)
    def _():
        pl.semaphore_signal(barrier, inc=1, device_id=(me, lev + 1), device_id_type=MESH)

    stacked = jnp.concatenate(
        [ref[m].astype(jnp.float32) for ref in (traj_ref, inc_ref) for m in range(tracers)], axis=0
    ).astype(jnp.bfloat16)
    for t in range(tiles):
        fields[t] = stacked[:, t * LANES : (t + 1) * LANES]
    for t in range(tiles, fields.shape[0]):
        fields[t] = jnp.zeros((2 * rows, LANES), jnp.bfloat16)
    vertical = vertical_ref[...]
    coef[pl.ds(0, 1), pl.ds(LANES, cols)] = courant_ref[...]
    coef[pl.ds(1, 1), pl.ds(LANES, cols)] = offset_ref[...].astype(jnp.float32)
    coef[pl.ds(2, 1), pl.ds(LANES, cols)] = jnp.maximum(vertical, 0.0)
    coef[pl.ds(3, 1), pl.ds(LANES, cols)] = jnp.maximum(-vertical, 0.0)
    coef[pl.ds(4, 4), pl.ds(LANES, cols)] = jnp.zeros((4, cols), jnp.float32)
    up_out[pl.ds(6, 2), :] = jnp.zeros((2, cols), jnp.float32)
    down_out[pl.ds(6, 2), :] = jnp.zeros((2, cols), jnp.float32)

    @pl.when(lev == 0)
    def _():
        below_in[...] = jnp.zeros_like(below_in)

    @pl.when(lev == n_lev - 1)
    def _():
        above_in[...] = jnp.zeros_like(above_in)

    placed[:, pl.ds(0, 1)] = jnp.zeros((reach, 1, rows, LANES), jnp.float32)
    placed[:, pl.ds(placed.shape[1] - 1, 1)] = jnp.zeros((reach, 1, rows, LANES), jnp.float32)

    starts = []
    total = jnp.int32(0)
    for d in range(reach):
        starts.append(total)
        total = total + counts_ref[0, d]

    firsts = [lax.shift_right_logical(start, 7) for start in starts]
    shifts = [lax.bitwise_and(start, LANES - 1) for start in starts]
    parts = cap // LANES
    lane = lax.broadcasted_iota(jnp.int32, (2 * rows, LANES), 1)
    skew = lax.broadcasted_iota(jnp.int32, (2 * LANES, LANES), 0) - lax.broadcasted_iota(
        jnp.int32, (2 * LANES, LANES), 1
    )

    def selection(amount):
        return jnp.where(skew == amount, 1.0, 0.0).astype(jnp.bfloat16)

    def slots_of(d):
        loaded = [fields[firsts[d] + t] for t in range(parts + 1)]
        pairs = [jnp.concatenate([loaded[t], loaded[t + 1]], axis=1) for t in range(parts)]
        moved = jnp.dot(
            jnp.concatenate(pairs, axis=0), selection(shifts[d]), preferred_element_type=jnp.float32
        )
        pieces = []
        for t in range(parts):
            value = moved[t * 2 * rows : (t + 1) * 2 * rows]
            pieces.append(jnp.where(lane + t * LANES < counts_ref[0, d], value, 0.0).astype(jnp.bfloat16))
        return jnp.concatenate(pieces, axis=1)

    tall = lax.broadcasted_iota(jnp.int32, (win, LANES), 1)

    def place_weight(d):
        chosen = selection(LANES - shifts[d])
        nothing = jnp.zeros((win, LANES), jnp.bfloat16)
        live = []
        for t in range(parts):
            piece = weight[d, :, pl.ds(t * LANES, LANES)]
            live.append(jnp.where(tall + t * LANES < counts_ref[0, d], piece, nothing))
        live = [nothing, *live, nothing]
        for t in range(parts + 1):
            moved = jnp.dot(
                jnp.concatenate([live[t], live[t + 1]], axis=1), chosen, preferred_element_type=jnp.float32
            )
            shifted[d, :, pl.ds(t * LANES, LANES)] = moved.astype(jnp.bfloat16)

    forward = {
        d: pltpu.make_async_remote_copy(
            src_ref=outgoing.at[d],
            dst_ref=recv.at[d],
            send_sem=fwd_send.at[d],
            recv_sem=fwd_recv.at[d],
            device_id=tile_at(d - centre),
            device_id_type=MESH,
        )
        for d in range(reach)
        if d != centre
    }
    giving = {
        d: pltpu.make_async_remote_copy(
            src_ref=adj.at[:, pl.ds(d * span, win)],
            dst_ref=back.at[d],
            send_sem=ret_send.at[d],
            recv_sem=ret_recv.at[d],
            device_id=tile_at(centre - d),
            device_id_type=MESH,
        )
        for d in range(reach)
        if d != centre
    }

    def edges(ref, send_sem, recv_sem, base):
        left = pltpu.make_async_remote_copy(
            src_ref=ref.at[:, pl.ds(LANES, LANES)],
            dst_ref=ref.at[:, pl.ds(LANES + cols, LANES)],
            send_sem=send_sem.at[base],
            recv_sem=recv_sem.at[base],
            device_id=tile_at(-1),
            device_id_type=MESH,
        )
        right = pltpu.make_async_remote_copy(
            src_ref=ref.at[:, pl.ds(cols, LANES)],
            dst_ref=ref.at[:, pl.ds(0, LANES)],
            send_sem=send_sem.at[base + 1],
            recv_sem=recv_sem.at[base + 1],
            device_id=tile_at(1),
            device_id_type=MESH,
        )
        return left, right

    coef_edges = edges(coef, coef_send, coef_recv, 0)
    delta_edges = edges(delta, col_send, col_recv, 0)
    tang_edges = edges(tang, col_send, col_recv, 2)

    stage_ranges = (
        ((0, 1), (tiles - 1, tiles)),
        ((1, 5), (11, tiles - 1)),
        ((5, 11),),
    )
    level_up, level_down = {}, {}
    index = 0
    for ranges in stage_ranges:
        for lo, hi in ranges:
            part = pl.ds(lo * LANES, (hi - lo) * LANES)
            level_up[lo, hi] = pltpu.make_async_remote_copy(
                src_ref=up_out.at[:, part],
                dst_ref=below_in.at[:, part],
                send_sem=lev_send.at[index],
                recv_sem=lev_recv.at[index],
                device_id=(me, lax.rem(lev + 1, n_lev)),
                device_id_type=MESH,
            )
            level_down[lo, hi] = pltpu.make_async_remote_copy(
                src_ref=down_out.at[:, part],
                dst_ref=above_in.at[:, part],
                send_sem=lev_send.at[index + 1],
                recv_sem=lev_recv.at[index + 1],
                device_id=(me, lax.rem(lev + n_lev - 1, n_lev)),
                device_id_type=MESH,
            )
            index += 2

    def level_start(stage):
        @pl.when(lev < n_lev - 1)
        def _():
            for key in stage_ranges[stage]:
                level_up[key].start()

        @pl.when(lev > 0)
        def _():
            for key in stage_ranges[stage]:
                level_down[key].start()

    def level_wait(stage):
        @pl.when(lev > 0)
        def _():
            for key in stage_ranges[stage]:
                level_up[key].wait_recv()

        @pl.when(lev < n_lev - 1)
        def _():
            for key in stage_ranges[stage]:
                level_down[key].wait_recv()

    for position, d in enumerate(SEND_ORDER):
        slotted = slots_of(d)
        weight_copies[d].wait()
        window = lax.dot_general(
            slotted, weight[d], (((1,), (1,)), ((), ())), preferred_element_type=jnp.float32
        )
        if d == centre:
            recv[d] = window
        else:
            outgoing[d] = window
            if position == 0:
                pl.semaphore_wait(
                    barrier,
                    2 * centre + (lev > 0).astype(jnp.int32) + (lev < n_lev - 1).astype(jnp.int32),
                )
            forward[d].start()
            if position == 0:
                for copy in coef_edges:
                    copy.start()

    def finish_block(b):
        value = recv[b, :, pl.ds(0, span)] + recv[(b - 1) % reach, :, pl.ds(span, span)]
        for m in range(tracers):
            part = pl.ds(m * levels, levels)
            loss[part, pl.ds(b * span, span)] = 2.0 * kappa_ref[m] * value[m * levels : (m + 1) * levels]
        delta[:, pl.ds(LANES + b * span, span)] = value[rows:]

    def level_rows(width):
        return lax.broadcasted_iota(jnp.int32, (levels, width), 0)

    def tangent_partial(lo, hi):
        width = (hi - lo) * LANES
        own = pl.ds(LANES + lo * LANES, width)
        courant, offset = coef[pl.ds(0, 1), own], coef[pl.ds(1, 1), own]
        rising, sinking = coef[pl.ds(2, 1), own], coef[pl.ds(3, 1), own]
        level = level_rows(width)
        for m in range(tracers):
            part = pl.ds(m * levels, levels)
            wide = delta[part, pl.ds(lo * LANES, width + 2 * LANES)]
            here = wide[:, LANES : LANES + width]
            departed = jnp.zeros_like(here)
            for shift in range(-HALO, HALO + 1):
                moved = here
                if shift != 0:
                    moved = pltpu.roll(wide, (-shift) % (width + 2 * LANES), 1)[:, LANES : LANES + width]
                departed = jnp.where(offset == float(shift), moved, departed)
            below = jnp.where(level == 0, 0.0, pltpu.roll(here, 1, 0))
            above = jnp.where(level == levels - 1, 0.0, pltpu.roll(here, levels - 1, 0))
            value = (
                here
                + courant * (departed - here)
                + rising * (below - here)
                + sinking * (above - here)
                - loss[part, pl.ds(lo * LANES, width)] * here
            )
            tang[part, own] = value
            out = pl.ds(lo * LANES, width)
            up_out[pl.ds(m, 1), out] = value[levels - 1 : levels]
            up_out[pl.ds(tracers + m, 1), out] = here[levels - 1 : levels]
            down_out[pl.ds(m, 1), out] = value[0:1]
            down_out[pl.ds(tracers + m, 1), out] = here[0:1]

    def tangent_finish(lo, hi):
        width = (hi - lo) * LANES
        own = pl.ds(LANES + lo * LANES, width)
        out = pl.ds(lo * LANES, width)
        rising, sinking = coef[pl.ds(2, 1), own], coef[pl.ds(3, 1), own]
        level = level_rows(width)
        for m in range(tracers):
            part = pl.ds(m * levels, levels)
            value = tang[part, own]
            value = value + jnp.where(level == 0, rising * below_in[pl.ds(tracers + m, 1), out], 0.0)
            value = value + jnp.where(level == levels - 1, sinking * above_in[pl.ds(tracers + m, 1), out], 0.0)
            tang[part, own] = value
            tangent_out[m, :, out] = value

    def adjoint(lo, hi):
        width = (hi - lo) * LANES
        own = pl.ds(LANES + lo * LANES, width)
        out = pl.ds(lo * LANES, width)
        around = pl.ds(lo * LANES, width + 2 * LANES)
        courant, rising, sinking = coef[pl.ds(0, 1), own], coef[pl.ds(2, 1), own], coef[pl.ds(3, 1), own]
        wide_courant, wide_offset = coef[pl.ds(0, 1), around], coef[pl.ds(1, 1), around]
        level = level_rows(width)
        pieces = []
        for m in range(tracers):
            part = pl.ds(m * levels, levels)
            wide = tang[part, around]
            here = wide[:, LANES : LANES + width]
            arrived = jnp.zeros_like(here)
            for shift in range(-HALO, HALO + 1):
                term = jnp.where(wide_offset == float(shift), wide_courant, 0.0) * wide
                if shift != 0:
                    term = pltpu.roll(term, shift % (width + 2 * LANES), 1)
                arrived = arrived + term[:, LANES : LANES + width]
            own_delta = delta[part, own]
            under = below_in[pl.ds(m, 1), out] + sinking * own_delta[0:1]
            over = above_in[pl.ds(m, 1), out] + rising * own_delta[levels - 1 : levels]
            under = jnp.where(lev > 0, under, 0.0)
            over = jnp.where(lev < n_lev - 1, over, 0.0)
            lower = jnp.where(level == 0, under, pltpu.roll(here, 1, 0))
            upper = jnp.where(level == levels - 1, over, pltpu.roll(here, levels - 1, 0))
            diagonal = 1.0 - courant - rising - sinking - loss[part, out]
            pieces.append(diagonal * here + arrived + rising * upper + sinking * lower)
        value = jnp.concatenate(pieces, axis=0).astype(jnp.bfloat16)
        adj[:, out] = value
        if lo == 0:
            adj[:, pl.ds(cols, span)] = value[:, :span]

    for d in range(reach):
        place_weight(d)
    for d in (0, 7, 6):
        forward[d].wait_recv()
    finish_block(0)
    finish_block(7)
    for copy in delta_edges:
        copy.start()
    for copy in (*delta_edges, *coef_edges):
        copy.wait_recv()
    for lo, hi in stage_ranges[0]:
        tangent_partial(lo, hi)
    level_start(0)
    for d in (1, 5, 2):
        forward[d].wait_recv()
    for b in (1, 6, 2, 5):
        finish_block(b)
    for lo, hi in stage_ranges[1]:
        tangent_partial(lo, hi)
    level_start(1)
    level_wait(0)
    for lo, hi in stage_ranges[0]:
        tangent_finish(lo, hi)
    for copy in tang_edges:
        copy.start()
    forward[3].wait_recv()
    for b in (3, 4):
        finish_block(b)
    for lo, hi in stage_ranges[2]:
        tangent_partial(lo, hi)
    level_start(2)
    level_wait(1)
    for lo, hi in stage_ranges[1]:
        tangent_finish(lo, hi)
    for copy in tang_edges:
        copy.wait_recv()
    adjoint(0, 4)
    adjoint(12, tiles)
    for d in (0, 7, 6):
        giving[d].start()
    level_wait(2)
    for lo, hi in stage_ranges[2]:
        tangent_finish(lo, hi)
    adjoint(4, 12)
    for d in (1, 2, 5, 3):
        giving[d].start()

    for d in (centre, 0, 7, 6, 1, 2, 5, 3):
        if d == centre:
            returned = adj[:, pl.ds(d * span, win)]
        else:
            giving[d].wait_recv()
            returned = back[d]
        grad = jnp.dot(returned, shifted[d], preferred_element_type=jnp.float32)
        for t in range(parts + 1):
            placed[d, t + 1] = grad[:, t * LANES : (t + 1) * LANES]

    last = placed.shape[1] - 1
    for t in range(tiles):
        value = None
        for d in range(reach):
            at = lax.min(lax.max(t + 1 - firsts[d], 0), last)
            piece = placed[d, at]
            value = piece if value is None else value + piece
        for m in range(tracers):
            grad_out[m, :, pl.ds(t * LANES, LANES)] = value[m * levels : (m + 1) * levels]

    for copy in (*forward.values(), *giving.values(), *coef_edges, *delta_edges, *tang_edges):
        copy.wait_send()

    @pl.when(lev < n_lev - 1)
    def _():
        for copy in level_up.values():
            copy.wait_send()

    @pl.when(lev > 0)
    def _():
        for copy in level_down.values():
            copy.wait_send()


def shards(n_tile, n_lev, trajectory, increment, counts, remap_weight, kappa, courant, vertical, offset):
    tracers, levels, cols = trajectory.shape
    reach, win, cap = remap_weight.shape[1:]
    rows = tracers * levels
    span = cols // reach
    wide = cols + 2 * LANES
    f32, bf16 = jnp.float32, jnp.bfloat16
    vmem = pl.BlockSpec(memory_space=pltpu.VMEM)
    smem = pl.BlockSpec(memory_space=pltpu.SMEM)
    dma = pltpu.SemaphoreType.DMA
    out = jax.ShapeDtypeStruct((tracers, levels, cols), f32)
    return pl.pallas_call(
        functools.partial(kernel, n_tile, n_lev),
        out_shape=(out, out),
        in_specs=[vmem, vmem, smem, smem, vmem, vmem, vmem, pl.BlockSpec(memory_space=pl.ANY)],
        out_specs=(vmem, vmem),
        scratch_shapes=[
            pltpu.VMEM((reach, win, cap), bf16),
            pltpu.VMEM((reach, win, cap + LANES), bf16),
            pltpu.VMEM((cols // LANES + cap // LANES + 1, 2 * rows, LANES), bf16),
            pltpu.VMEM((reach, 2 * rows, win), f32),
            pltpu.VMEM((reach, 2 * rows, win), f32),
            pltpu.VMEM((8, wide), f32),
            pltpu.VMEM((rows, wide), f32),
            pltpu.VMEM((rows, cols), f32),
            pltpu.VMEM((rows, wide), f32),
            pltpu.VMEM((8, cols), f32),
            pltpu.VMEM((8, cols), f32),
            pltpu.VMEM((8, cols), f32),
            pltpu.VMEM((8, cols), f32),
            pltpu.VMEM((rows, cols + span), bf16),
            pltpu.VMEM((reach, rows, win), bf16),
            pltpu.VMEM((reach, cap // LANES + 3, rows, LANES), f32),
            dma((reach,)),
            dma((reach,)),
            dma((reach,)),
            dma((2,)),
            dma((2,)),
            dma((4,)),
            dma((4,)),
            dma((10,)),
            dma((10,)),
            dma((reach,)),
            dma((reach,)),
        ],
        compiler_params=pltpu.CompilerParams(
            collective_id=0, has_side_effects=True, vmem_limit_bytes=60 * 1024 * 1024
        ),
    )(
        trajectory,
        increment,
        counts,
        kappa,
        courant.reshape(1, cols),
        vertical.reshape(1, cols),
        offset.reshape(1, cols),
        remap_weight,
    )


def solution(mesh):
    return jax.shard_map(
        functools.partial(shards, mesh.shape["tile"], mesh.shape["lev"]),
        mesh=mesh,
        in_specs=(
            P(None, "lev", "tile"),
            P(None, "lev", "tile"),
            P("tile", None),
            P("tile", None, None, None),
            P(),
            P("tile"),
            P("tile"),
            P("tile"),
        ),
        out_specs=(P(None, "lev", "tile"), P(None, "lev", "tile")),
        check_vma=False,
    )
```

```python
import functools

import jax
import jax.numpy as jnp
from jax import lax
from jax.experimental import pallas as pl
from jax.experimental.pallas import tpu as pltpu
from jax.sharding import PartitionSpec as P

MESH = pl.DeviceIdType.MESH
LANES = 128
HALO = 2
SEND_ORDER = (0, 7, 1, 6, 2, 5, 3, 4)


def kernel(
    n_tile,
    n_lev,
    traj_hbm,
    inc_hbm,
    counts_hbm,
    kappa_hbm,
    courant_hbm,
    vertical_hbm,
    offset_hbm,
    weight_hbm,
    tangent_out,
    grad_out,
    traj_ref,
    inc_ref,
    counts_ref,
    kappa_ref,
    courant_ref,
    vertical_ref,
    offset_ref,
    weight,
    shifted,
    fields,
    outgoing,
    recv,
    coef,
    delta,
    loss,
    tang,
    up_out,
    down_out,
    below_in,
    above_in,
    adj,
    back,
    placed,
    load_sem,
    weight_sem,
    fwd_send,
    fwd_recv,
    coef_send,
    coef_recv,
    col_send,
    col_recv,
    lev_send,
    lev_recv,
    ret_send,
    ret_recv,
):
    tracers, levels, cols = traj_hbm.shape
    rows = tracers * levels
    reach = weight_hbm.shape[1]
    win, cap = weight_hbm.shape[2], weight_hbm.shape[3]
    centre = reach // 2
    span = cols // reach
    tiles = cols // LANES
    sub = span // LANES
    me = lax.axis_index("tile")
    lev = lax.axis_index("lev")

    def tile_at(distance):
        return (lax.rem(me + (n_tile + distance), n_tile), lev)

    barrier = pltpu.get_barrier_semaphore()
    for distance in range(-centre, centre + 1):
        if distance != 0:
            pl.semaphore_signal(barrier, inc=1, device_id=tile_at(distance), device_id_type=MESH)

    @pl.when(lev > 0)
    def _():
        pl.semaphore_signal(barrier, inc=1, device_id=(me, lev - 1), device_id_type=MESH)

    @pl.when(lev < n_lev - 1)
    def _():
        pl.semaphore_signal(barrier, inc=1, device_id=(me, lev + 1), device_id_type=MESH)

    loads = [
        pltpu.make_async_copy(source, target, load_sem.at[i])
        for i, (source, target) in enumerate(
            (
                (counts_hbm, counts_ref),
                (kappa_hbm, kappa_ref),
                (traj_hbm, traj_ref),
                (inc_hbm, inc_ref),
                (courant_hbm, courant_ref),
                (vertical_hbm, vertical_ref),
                (offset_hbm, offset_ref),
            )
        )
    ]
    weight_copies = [
        pltpu.make_async_copy(weight_hbm.at[0, d], weight.at[d], weight_sem.at[d]) for d in range(reach)
    ]
    for copy in loads:
        copy.start()
    for d in SEND_ORDER:
        weight_copies[d].start()

    for copy in loads:
        copy.wait()
    stacked = jnp.concatenate(
        [ref[m].astype(jnp.float32) for ref in (traj_ref, inc_ref) for m in range(tracers)], axis=0
    ).astype(jnp.bfloat16)
    for t in range(tiles):
        fields[t] = stacked[:, t * LANES : (t + 1) * LANES]
    for t in range(tiles, fields.shape[0]):
        fields[t] = jnp.zeros((2 * rows, LANES), jnp.bfloat16)
    vertical = vertical_ref[...]
    coef[pl.ds(0, 1), pl.ds(LANES, cols)] = courant_ref[...]
    coef[pl.ds(1, 1), pl.ds(LANES, cols)] = offset_ref[...].astype(jnp.float32)
    coef[pl.ds(2, 1), pl.ds(LANES, cols)] = jnp.maximum(vertical, 0.0)
    coef[pl.ds(3, 1), pl.ds(LANES, cols)] = jnp.maximum(-vertical, 0.0)
    coef[pl.ds(4, 4), pl.ds(LANES, cols)] = jnp.zeros((4, cols), jnp.float32)
    up_out[pl.ds(6, 2), :] = jnp.zeros((2, cols), jnp.float32)
    down_out[pl.ds(6, 2), :] = jnp.zeros((2, cols), jnp.float32)

    @pl.when(lev == 0)
    def _():
        below_in[...] = jnp.zeros_like(below_in)

    @pl.when(lev == n_lev - 1)
    def _():
        above_in[...] = jnp.zeros_like(above_in)

    placed[:, pl.ds(0, 1)] = jnp.zeros((reach, 1, rows, LANES), jnp.float32)
    placed[:, pl.ds(placed.shape[1] - 1, 1)] = jnp.zeros((reach, 1, rows, LANES), jnp.float32)

    starts = []
    total = jnp.int32(0)
    for d in range(reach):
        starts.append(total)
        total = total + counts_ref[0, d]

    firsts = [lax.shift_right_logical(start, 7) for start in starts]
    shifts = [lax.bitwise_and(start, LANES - 1) for start in starts]
    parts = cap // LANES
    lane = lax.broadcasted_iota(jnp.int32, (2 * rows, LANES), 1)
    skew = lax.broadcasted_iota(jnp.int32, (2 * LANES, LANES), 0) - lax.broadcasted_iota(
        jnp.int32, (2 * LANES, LANES), 1
    )

    def selection(amount):
        return jnp.where(skew == amount, 1.0, 0.0).astype(jnp.bfloat16)

    def slots_of(d):
        loaded = [fields[firsts[d] + t] for t in range(parts + 1)]
        pairs = [jnp.concatenate([loaded[t], loaded[t + 1]], axis=1) for t in range(parts)]
        moved = jnp.dot(
            jnp.concatenate(pairs, axis=0), selection(shifts[d]), preferred_element_type=jnp.float32
        )
        pieces = []
        for t in range(parts):
            value = moved[t * 2 * rows : (t + 1) * 2 * rows]
            pieces.append(jnp.where(lane + t * LANES < counts_ref[0, d], value, 0.0).astype(jnp.bfloat16))
        return jnp.concatenate(pieces, axis=1)

    tall = lax.broadcasted_iota(jnp.int32, (win, LANES), 1)

    def place_weight(d):
        chosen = selection(LANES - shifts[d])
        nothing = jnp.zeros((win, LANES), jnp.bfloat16)
        live = []
        for t in range(parts):
            piece = weight[d, :, pl.ds(t * LANES, LANES)]
            live.append(jnp.where(tall + t * LANES < counts_ref[0, d], piece, nothing))
        live = [nothing, *live, nothing]
        for t in range(parts + 1):
            moved = jnp.dot(
                jnp.concatenate([live[t], live[t + 1]], axis=1), chosen, preferred_element_type=jnp.float32
            )
            shifted[d, :, pl.ds(t * LANES, LANES)] = moved.astype(jnp.bfloat16)

    forward = {
        d: pltpu.make_async_remote_copy(
            src_ref=outgoing.at[d],
            dst_ref=recv.at[d],
            send_sem=fwd_send.at[d],
            recv_sem=fwd_recv.at[d],
            device_id=tile_at(d - centre),
            device_id_type=MESH,
        )
        for d in range(reach)
        if d != centre
    }
    giving = {
        d: pltpu.make_async_remote_copy(
            src_ref=adj.at[:, pl.ds(d * span, win)],
            dst_ref=back.at[d],
            send_sem=ret_send.at[d],
            recv_sem=ret_recv.at[d],
            device_id=tile_at(centre - d),
            device_id_type=MESH,
        )
        for d in range(reach)
        if d != centre
    }

    def edges(ref, send_sem, recv_sem, base):
        left = pltpu.make_async_remote_copy(
            src_ref=ref.at[:, pl.ds(LANES, LANES)],
            dst_ref=ref.at[:, pl.ds(LANES + cols, LANES)],
            send_sem=send_sem.at[base],
            recv_sem=recv_sem.at[base],
            device_id=tile_at(-1),
            device_id_type=MESH,
        )
        right = pltpu.make_async_remote_copy(
            src_ref=ref.at[:, pl.ds(cols, LANES)],
            dst_ref=ref.at[:, pl.ds(0, LANES)],
            send_sem=send_sem.at[base + 1],
            recv_sem=recv_sem.at[base + 1],
            device_id=tile_at(1),
            device_id_type=MESH,
        )
        return left, right

    coef_edges = edges(coef, coef_send, coef_recv, 0)
    delta_edges = edges(delta, col_send, col_recv, 0)
    tang_edges = edges(tang, col_send, col_recv, 2)

    stage_ranges = (
        ((0, 1), (tiles - 1, tiles)),
        ((1, 5), (11, tiles - 1)),
        ((5, 11),),
    )
    level_up, level_down = {}, {}
    index = 0
    for ranges in stage_ranges:
        for lo, hi in ranges:
            part = pl.ds(lo * LANES, (hi - lo) * LANES)
            level_up[lo, hi] = pltpu.make_async_remote_copy(
                src_ref=up_out.at[:, part],
                dst_ref=below_in.at[:, part],
                send_sem=lev_send.at[index],
                recv_sem=lev_recv.at[index],
                device_id=(me, lax.rem(lev + 1, n_lev)),
                device_id_type=MESH,
            )
            level_down[lo, hi] = pltpu.make_async_remote_copy(
                src_ref=down_out.at[:, part],
                dst_ref=above_in.at[:, part],
                send_sem=lev_send.at[index + 1],
                recv_sem=lev_recv.at[index + 1],
                device_id=(me, lax.rem(lev + n_lev - 1, n_lev)),
                device_id_type=MESH,
            )
            index += 2

    def level_start(stage):
        @pl.when(lev < n_lev - 1)
        def _():
            for key in stage_ranges[stage]:
                level_up[key].start()

        @pl.when(lev > 0)
        def _():
            for key in stage_ranges[stage]:
                level_down[key].start()

    def level_wait(stage):
        @pl.when(lev > 0)
        def _():
            for key in stage_ranges[stage]:
                level_up[key].wait_recv()

        @pl.when(lev < n_lev - 1)
        def _():
            for key in stage_ranges[stage]:
                level_down[key].wait_recv()

    for position, d in enumerate(SEND_ORDER):
        slotted = slots_of(d)
        weight_copies[d].wait()
        window = lax.dot_general(
            slotted, weight[d], (((1,), (1,)), ((), ())), preferred_element_type=jnp.float32
        )
        if d == centre:
            recv[d] = window
        else:
            outgoing[d] = window
            if position == 0:
                pl.semaphore_wait(
                    barrier,
                    2 * centre + (lev > 0).astype(jnp.int32) + (lev < n_lev - 1).astype(jnp.int32),
                )
            forward[d].start()
            if position == 0:
                for copy in coef_edges:
                    copy.start()

    def finish_block(b):
        value = recv[b, :, pl.ds(0, span)] + recv[(b - 1) % reach, :, pl.ds(span, span)]
        for m in range(tracers):
            part = pl.ds(m * levels, levels)
            loss[part, pl.ds(b * span, span)] = 2.0 * kappa_ref[m] * value[m * levels : (m + 1) * levels]
        delta[:, pl.ds(LANES + b * span, span)] = value[rows:]

    def level_rows(width):
        return lax.broadcasted_iota(jnp.int32, (levels, width), 0)

    def tangent_partial(lo, hi):
        width = (hi - lo) * LANES
        own = pl.ds(LANES + lo * LANES, width)
        courant, offset = coef[pl.ds(0, 1), own], coef[pl.ds(1, 1), own]
        rising, sinking = coef[pl.ds(2, 1), own], coef[pl.ds(3, 1), own]
        level = level_rows(width)
        for m in range(tracers):
            part = pl.ds(m * levels, levels)
            wide = delta[part, pl.ds(lo * LANES, width + 2 * LANES)]
            here = wide[:, LANES : LANES + width]
            departed = jnp.zeros_like(here)
            for shift in range(-HALO, HALO + 1):
                moved = here
                if shift != 0:
                    moved = pltpu.roll(wide, (-shift) % (width + 2 * LANES), 1)[:, LANES : LANES + width]
                departed = jnp.where(offset == float(shift), moved, departed)
            below = jnp.where(level == 0, 0.0, pltpu.roll(here, 1, 0))
            above = jnp.where(level == levels - 1, 0.0, pltpu.roll(here, levels - 1, 0))
            value = (
                here
                + courant * (departed - here)
                + rising * (below - here)
                + sinking * (above - here)
                - loss[part, pl.ds(lo * LANES, width)] * here
            )
            tang[part, own] = value
            out = pl.ds(lo * LANES, width)
            up_out[pl.ds(m, 1), out] = value[levels - 1 : levels]
            up_out[pl.ds(tracers + m, 1), out] = here[levels - 1 : levels]
            down_out[pl.ds(m, 1), out] = value[0:1]
            down_out[pl.ds(tracers + m, 1), out] = here[0:1]

    def tangent_finish(lo, hi):
        width = (hi - lo) * LANES
        own = pl.ds(LANES + lo * LANES, width)
        out = pl.ds(lo * LANES, width)
        rising, sinking = coef[pl.ds(2, 1), own], coef[pl.ds(3, 1), own]
        level = level_rows(width)
        for m in range(tracers):
            part = pl.ds(m * levels, levels)
            value = tang[part, own]
            value = value + jnp.where(level == 0, rising * below_in[pl.ds(tracers + m, 1), out], 0.0)
            value = value + jnp.where(level == levels - 1, sinking * above_in[pl.ds(tracers + m, 1), out], 0.0)
            tang[part, own] = value
            tangent_out[m, :, out] = value

    def adjoint(lo, hi):
        width = (hi - lo) * LANES
        own = pl.ds(LANES + lo * LANES, width)
        out = pl.ds(lo * LANES, width)
        around = pl.ds(lo * LANES, width + 2 * LANES)
        courant, rising, sinking = coef[pl.ds(0, 1), own], coef[pl.ds(2, 1), own], coef[pl.ds(3, 1), own]
        wide_courant, wide_offset = coef[pl.ds(0, 1), around], coef[pl.ds(1, 1), around]
        level = level_rows(width)
        pieces = []
        for m in range(tracers):
            part = pl.ds(m * levels, levels)
            wide = tang[part, around]
            here = wide[:, LANES : LANES + width]
            arrived = jnp.zeros_like(here)
            for shift in range(-HALO, HALO + 1):
                term = jnp.where(wide_offset == float(shift), wide_courant, 0.0) * wide
                if shift != 0:
                    term = pltpu.roll(term, shift % (width + 2 * LANES), 1)
                arrived = arrived + term[:, LANES : LANES + width]
            own_delta = delta[part, own]
            under = below_in[pl.ds(m, 1), out] + sinking * own_delta[0:1]
            over = above_in[pl.ds(m, 1), out] + rising * own_delta[levels - 1 : levels]
            under = jnp.where(lev > 0, under, 0.0)
            over = jnp.where(lev < n_lev - 1, over, 0.0)
            lower = jnp.where(level == 0, under, pltpu.roll(here, 1, 0))
            upper = jnp.where(level == levels - 1, over, pltpu.roll(here, levels - 1, 0))
            diagonal = 1.0 - courant - rising - sinking - loss[part, out]
            pieces.append(diagonal * here + arrived + rising * upper + sinking * lower)
        value = jnp.concatenate(pieces, axis=0).astype(jnp.bfloat16)
        adj[:, out] = value
        if lo == 0:
            adj[:, pl.ds(cols, span)] = value[:, :span]

    for d in range(reach):
        place_weight(d)
    for d in (0, 7, 6):
        forward[d].wait_recv()
    finish_block(0)
    finish_block(7)
    for copy in delta_edges:
        copy.start()
    for copy in (*delta_edges, *coef_edges):
        copy.wait_recv()
    for lo, hi in stage_ranges[0]:
        tangent_partial(lo, hi)
    level_start(0)
    for d in (1, 5, 2):
        forward[d].wait_recv()
    for b in (1, 6, 2, 5):
        finish_block(b)
    for lo, hi in stage_ranges[1]:
        tangent_partial(lo, hi)
    level_start(1)
    level_wait(0)
    for lo, hi in stage_ranges[0]:
        tangent_finish(lo, hi)
    for copy in tang_edges:
        copy.start()
    forward[3].wait_recv()
    for b in (3, 4):
        finish_block(b)
    for lo, hi in stage_ranges[2]:
        tangent_partial(lo, hi)
    level_start(2)
    level_wait(1)
    for lo, hi in stage_ranges[1]:
        tangent_finish(lo, hi)
    for copy in tang_edges:
        copy.wait_recv()
    adjoint(0, 4)
    adjoint(12, tiles)
    for d in (0, 7, 6):
        giving[d].start()
    level_wait(2)
    for lo, hi in stage_ranges[2]:
        tangent_finish(lo, hi)
    adjoint(4, 12)
    for d in (1, 2, 5, 3):
        giving[d].start()

    for d in (centre, 0, 7, 6, 1, 2, 5, 3):
        if d == centre:
            returned = adj[:, pl.ds(d * span, win)]
        else:
            giving[d].wait_recv()
            returned = back[d]
        grad = jnp.dot(returned, shifted[d], preferred_element_type=jnp.float32)
        for t in range(parts + 1):
            placed[d, t + 1] = grad[:, t * LANES : (t + 1) * LANES]

    last = placed.shape[1] - 1
    for t in range(tiles):
        value = None
        for d in range(reach):
            at = lax.min(lax.max(t + 1 - firsts[d], 0), last)
            piece = placed[d, at]
            value = piece if value is None else value + piece
        for m in range(tracers):
            grad_out[m, :, pl.ds(t * LANES, LANES)] = value[m * levels : (m + 1) * levels]

    for copy in (*forward.values(), *giving.values(), *coef_edges, *delta_edges, *tang_edges):
        copy.wait_send()

    @pl.when(lev < n_lev - 1)
    def _():
        for copy in level_up.values():
            copy.wait_send()

    @pl.when(lev > 0)
    def _():
        for copy in level_down.values():
            copy.wait_send()


def shards(n_tile, n_lev, trajectory, increment, counts, remap_weight, kappa, courant, vertical, offset):
    tracers, levels, cols = trajectory.shape
    reach, win, cap = remap_weight.shape[1:]
    rows = tracers * levels
    span = cols // reach
    wide = cols + 2 * LANES
    f32, bf16 = jnp.float32, jnp.bfloat16
    vmem = pl.BlockSpec(memory_space=pltpu.VMEM)
    dma = pltpu.SemaphoreType.DMA
    out = jax.ShapeDtypeStruct((tracers, levels, cols), f32)
    return pl.pallas_call(
        functools.partial(kernel, n_tile, n_lev),
        out_shape=(out, out),
        in_specs=[pl.BlockSpec(memory_space=pltpu.HBM)] * 8,
        out_specs=(vmem, vmem),
        scratch_shapes=[
            pltpu.VMEM((tracers, levels, cols), bf16),
            pltpu.VMEM((tracers, levels, cols), bf16),
            pltpu.SMEM((1, reach), jnp.int32),
            pltpu.SMEM((tracers,), f32),
            pltpu.VMEM((1, cols), f32),
            pltpu.VMEM((1, cols), f32),
            pltpu.VMEM((1, cols), jnp.int32),
            pltpu.VMEM((reach, win, cap), bf16),
            pltpu.VMEM((reach, win, cap + LANES), bf16),
            pltpu.VMEM((cols // LANES + cap // LANES + 1, 2 * rows, LANES), bf16),
            pltpu.VMEM((reach, 2 * rows, win), f32),
            pltpu.VMEM((reach, 2 * rows, win), f32),
            pltpu.VMEM((8, wide), f32),
            pltpu.VMEM((rows, wide), f32),
            pltpu.VMEM((rows, cols), f32),
            pltpu.VMEM((rows, wide), f32),
            pltpu.VMEM((8, cols), f32),
            pltpu.VMEM((8, cols), f32),
            pltpu.VMEM((8, cols), f32),
            pltpu.VMEM((8, cols), f32),
            pltpu.VMEM((rows, cols + span), bf16),
            pltpu.VMEM((reach, rows, win), bf16),
            pltpu.VMEM((reach, cap // LANES + 3, rows, LANES), f32),
            dma((7,)),
            dma((reach,)),
            dma((reach,)),
            dma((reach,)),
            dma((2,)),
            dma((2,)),
            dma((4,)),
            dma((4,)),
            dma((10,)),
            dma((10,)),
            dma((reach,)),
            dma((reach,)),
        ],
        compiler_params=pltpu.CompilerParams(
            collective_id=0, has_side_effects=True, vmem_limit_bytes=24 * 1024 * 1024
        ),
    )(
        *(
            pltpu.with_memory_space_constraint(operand, pltpu.HBM)
            for operand in (
                trajectory,
                increment,
                counts,
                kappa,
                courant.reshape(1, cols),
                vertical.reshape(1, cols),
                offset.reshape(1, cols),
                remap_weight,
            )
        )
    )


def solution(mesh):
    return jax.shard_map(
        functools.partial(shards, mesh.shape["tile"], mesh.shape["lev"]),
        mesh=mesh,
        in_specs=(
            P(None, "lev", "tile"),
            P(None, "lev", "tile"),
            P("tile", None),
            P("tile", None, None, None),
            P(),
            P("tile"),
            P("tile"),
            P("tile"),
        ),
        out_specs=(P(None, "lev", "tile"), P(None, "lev", "tile")),
        check_vma=False,
    )
```

```python
import functools

import jax
import jax.numpy as jnp
from jax import lax
from jax.experimental import pallas as pl
from jax.experimental.pallas import tpu as pltpu
from jax.sharding import PartitionSpec as P

MESH = pl.DeviceIdType.MESH
LANES = 128
HALO = 2
SEND_ORDER = (0, 7, 6, 1, 2, 3, 5, 4)
EVEN, ODD = (0,), (1,)
BOTH = (0, 1)


def kernel(
    n_tile,
    n_lev,
    traj_hbm,
    inc_hbm,
    counts_hbm,
    kappa_hbm,
    courant_hbm,
    vertical_hbm,
    offset_hbm,
    weight_hbm,
    tangent_out,
    grad_out,
    traj_ref,
    inc_ref,
    counts_ref,
    kappa_ref,
    courant_ref,
    vertical_ref,
    offset_ref,
    weight,
    shifted,
    fields,
    outgoing,
    mixing,
    summed,
    recv,
    coef,
    delta,
    loss,
    tang,
    up_out,
    down_out,
    below_in,
    above_in,
    edge_up,
    edge_down,
    edge_below,
    edge_above,
    edge_tang,
    adj,
    back,
    placed,
    load_sem,
    weight_sem,
    fwd_send,
    fwd_recv,
    coef_send,
    coef_recv,
    col_send,
    col_recv,
    lev_send,
    lev_recv,
    ret_send,
    ret_recv,
):
    tracers, levels, cols = traj_hbm.shape
    rows = tracers * levels
    reach = weight_hbm.shape[1]
    win, cap = weight_hbm.shape[2], weight_hbm.shape[3]
    centre = reach // 2
    span = cols // reach
    tiles = cols // LANES
    sub = span // LANES
    me = lax.axis_index("tile")
    lev = lax.axis_index("lev")

    def tile_at(distance):
        return (lax.rem(me + (n_tile + distance), n_tile), lev)

    barrier = pltpu.get_barrier_semaphore()
    for distance in range(-centre, centre + 1):
        if distance != 0:
            pl.semaphore_signal(barrier, inc=1, device_id=tile_at(distance), device_id_type=MESH)

    @pl.when(lev > 0)
    def _():
        pl.semaphore_signal(barrier, inc=1, device_id=(me, lev - 1), device_id_type=MESH)

    @pl.when(lev < n_lev - 1)
    def _():
        pl.semaphore_signal(barrier, inc=1, device_id=(me, lev + 1), device_id_type=MESH)

    loads = [
        pltpu.make_async_copy(source, target, load_sem.at[i])
        for i, (source, target) in enumerate(
            (
                (counts_hbm, counts_ref),
                (kappa_hbm, kappa_ref),
                (traj_hbm, traj_ref),
                (inc_hbm, inc_ref),
                (courant_hbm, courant_ref),
                (vertical_hbm, vertical_ref),
                (offset_hbm, offset_ref),
            )
        )
    ]
    weight_copies = [
        pltpu.make_async_copy(weight_hbm.at[0, d], weight.at[d], weight_sem.at[d]) for d in range(reach)
    ]
    for copy in loads:
        copy.start()
    for d in SEND_ORDER:
        weight_copies[d].start()

    for copy in loads:
        copy.wait()
    stacked = jnp.concatenate(
        [ref[m].astype(jnp.float32) for ref in (traj_ref, inc_ref) for m in range(tracers)], axis=0
    ).astype(jnp.bfloat16)
    for t in range(tiles):
        fields[t] = stacked[:, t * LANES : (t + 1) * LANES]
    for t in range(tiles, fields.shape[0]):
        fields[t] = jnp.zeros((2 * rows, LANES), jnp.bfloat16)
    vertical = vertical_ref[...]
    coef[pl.ds(0, 1), pl.ds(LANES, cols)] = courant_ref[...]
    coef[pl.ds(1, 1), pl.ds(LANES, cols)] = offset_ref[...].astype(jnp.float32)
    coef[pl.ds(2, 1), pl.ds(LANES, cols)] = jnp.maximum(vertical, 0.0)
    coef[pl.ds(3, 1), pl.ds(LANES, cols)] = jnp.maximum(-vertical, 0.0)
    coef[pl.ds(4, 4), pl.ds(LANES, cols)] = jnp.zeros((4, cols), jnp.float32)
    for ref in (up_out, down_out, edge_up, edge_down):
        ref[pl.ds(6, 2), :] = jnp.zeros((2, ref.shape[1]), jnp.float32)

    @pl.when(lev == 0)
    def _():
        below_in[...] = jnp.zeros_like(below_in)
        edge_below[...] = jnp.zeros_like(edge_below)

    @pl.when(lev == n_lev - 1)
    def _():
        above_in[...] = jnp.zeros_like(above_in)
        edge_above[...] = jnp.zeros_like(edge_above)

    placed[:, pl.ds(0, 1)] = jnp.zeros((reach, 1, rows, LANES), jnp.float32)
    placed[:, pl.ds(placed.shape[1] - 1, 1)] = jnp.zeros((reach, 1, rows, LANES), jnp.float32)

    starts = []
    total = jnp.int32(0)
    for d in range(reach):
        starts.append(total)
        total = total + counts_ref[0, d]

    firsts = [lax.shift_right_logical(start, 7) for start in starts]
    shifts = [lax.bitwise_and(start, LANES - 1) for start in starts]
    parts = cap // LANES
    lane = lax.broadcasted_iota(jnp.int32, (2 * rows, LANES), 1)
    skew = lax.broadcasted_iota(jnp.int32, (2 * LANES, LANES), 0) - lax.broadcasted_iota(
        jnp.int32, (2 * LANES, LANES), 1
    )

    def selection(amount):
        return jnp.where(skew == amount, 1.0, 0.0).astype(jnp.bfloat16)

    def slots_of(d):
        loaded = [fields[firsts[d] + t] for t in range(parts + 1)]
        pairs = [jnp.concatenate([loaded[t], loaded[t + 1]], axis=1) for t in range(parts)]
        moved = jnp.dot(
            jnp.concatenate(pairs, axis=0), selection(shifts[d]), preferred_element_type=jnp.float32
        )
        pieces = []
        for t in range(parts):
            value = moved[t * 2 * rows : (t + 1) * 2 * rows]
            pieces.append(jnp.where(lane + t * LANES < counts_ref[0, d], value, 0.0).astype(jnp.bfloat16))
        return jnp.concatenate(pieces, axis=1)

    tall = lax.broadcasted_iota(jnp.int32, (win, LANES), 1)

    def place_weight(d):
        chosen = selection(LANES - shifts[d])
        nothing = jnp.zeros((win, LANES), jnp.bfloat16)
        live = []
        for t in range(parts):
            piece = weight[d, :, pl.ds(t * LANES, LANES)]
            live.append(jnp.where(tall + t * LANES < counts_ref[0, d], piece, nothing))
        live = [nothing, *live, nothing]
        for t in range(parts + 1):
            moved = jnp.dot(
                jnp.concatenate([live[t], live[t + 1]], axis=1), chosen, preferred_element_type=jnp.float32
            )
            shifted[d, :, pl.ds(t * LANES, LANES)] = moved.astype(jnp.bfloat16)

    parity = lax.rem(me, 2)
    half = win // 2

    def on_core(cores, run):
        if len(cores) == 2:
            run()
        else:
            pl.when(parity == cores[0])(run)

    def window_part(d, lane, width):
        part = pl.ds(lane, width)
        return outgoing.at[d, :, part], recv.at[d, :, part], d - centre

    plan = {
        "e0": (BOTH, *window_part(0, 0, LANES)),
        "e7": (BOTH, *window_part(7, LANES, 2 * LANES)),
        "e6": (BOTH, *window_part(6, 3 * LANES, LANES)),
        "g0w": (EVEN, *window_part(0, LANES, 3 * LANES)),
        "g0l": (ODD, *window_part(0, LANES, LANES)),
        "g7z": (BOTH, *window_part(7, 3 * LANES, LANES)),
        "g7a": (ODD, *window_part(7, 0, LANES)),
        "g6m": (EVEN, *window_part(6, half, LANES)),
        "g6l": (ODD, *window_part(6, 0, half)),
        "g1h": (EVEN, *window_part(1, half, half)),
        "g1l": (ODD, *window_part(1, 0, half)),
        "g2h": (EVEN, *window_part(2, half, half)),
        "g2l": (ODD, *window_part(2, 0, half)),
        "g3h": (EVEN, *window_part(3, half, half)),
        "g3w": (ODD, *window_part(3, 0, win)),
        "g5w": (EVEN, *window_part(5, 0, win)),
        "g5l": (ODD, *window_part(5, 0, half)),
        "m1": (EVEN, outgoing.at[1, :, pl.ds(0, half)], mixing.at[0], 1),
        "m2": (EVEN, outgoing.at[2, :, pl.ds(0, half)], mixing.at[1], 1),
        "m3": (EVEN, outgoing.at[3, :, pl.ds(0, half)], mixing.at[2], 1),
        "m5": (ODD, outgoing.at[5, :, pl.ds(half, half)], mixing.at[0], -1),
        "m6": (ODD, outgoing.at[6, :, pl.ds(half, LANES)], mixing.at[1, :, pl.ds(0, LANES)], -1),
        "c1": (ODD, summed.at[0], recv.at[1, :, pl.ds(0, half)], -4),
        "c2": (ODD, summed.at[1], recv.at[2, :, pl.ds(0, half)], -3),
        "c3": (ODD, summed.at[2], recv.at[3, :, pl.ds(0, half)], -2),
        "c6": (EVEN, summed.at[0], recv.at[6, :, pl.ds(0, half)], 2),
        "c7": (EVEN, summed.at[1, :, pl.ds(0, LANES)], recv.at[7, :, pl.ds(0, LANES)], 3),
    }
    forward = {
        name: pltpu.make_async_remote_copy(
            src_ref=source,
            dst_ref=target,
            send_sem=fwd_send.at[i],
            recv_sem=fwd_recv.at[i],
            device_id=tile_at(distance),
            device_id_type=MESH,
        )
        for i, (name, (_, source, target, distance)) in enumerate(plan.items())
    }

    def send(*names):
        for name in names:
            on_core(plan[name][0], forward[name].start)

    def arrived(*names):
        for name in names:
            forward[name].wait_recv()

    giving = {
        d: pltpu.make_async_remote_copy(
            src_ref=adj.at[:, pl.ds(d * span, win)],
            dst_ref=back.at[d],
            send_sem=ret_send.at[d],
            recv_sem=ret_recv.at[d],
            device_id=tile_at(centre - d),
            device_id_type=MESH,
        )
        for d in range(reach)
        if d != centre
    }

    def edges(first, last, ref, send_sem, recv_sem, base):
        left = pltpu.make_async_remote_copy(
            src_ref=first,
            dst_ref=ref.at[:, pl.ds(LANES + cols, LANES)],
            send_sem=send_sem.at[base],
            recv_sem=recv_sem.at[base],
            device_id=tile_at(-1),
            device_id_type=MESH,
        )
        right = pltpu.make_async_remote_copy(
            src_ref=last,
            dst_ref=ref.at[:, pl.ds(0, LANES)],
            send_sem=send_sem.at[base + 1],
            recv_sem=recv_sem.at[base + 1],
            device_id=tile_at(1),
            device_id_type=MESH,
        )
        return left, right

    first_tile, last_tile = pl.ds(LANES, LANES), pl.ds(cols, LANES)
    coef_edges = edges(coef.at[:, first_tile], coef.at[:, last_tile], coef, coef_send, coef_recv, 0)
    delta_edges = edges(delta.at[:, first_tile], delta.at[:, last_tile], delta, col_send, col_recv, 0)
    tang_edges = edges(
        edge_tang.at[:, pl.ds(LANES, LANES)], edge_tang.at[:, pl.ds(0, LANES)], tang, col_send, col_recv, 2
    )

    early = ((0, 5), (11, tiles))
    late = ((5, 11),)
    everything = ((0, 2),)
    stages = (
        (everything, edge_up, edge_down, edge_below, edge_above),
        (early, up_out, down_out, below_in, above_in),
        (late, up_out, down_out, below_in, above_in),
    )
    level_up, level_down = ([], [], []), ([], [], [])
    index = 0
    for stage, (ranges, up_from, down_from, up_to, down_to) in enumerate(stages):
        for lo, hi in ranges:
            part = pl.ds(lo * LANES, (hi - lo) * LANES)
            level_up[stage].append(
                pltpu.make_async_remote_copy(
                    src_ref=up_from.at[:, part],
                    dst_ref=up_to.at[:, part],
                    send_sem=lev_send.at[index],
                    recv_sem=lev_recv.at[index],
                    device_id=(me, lax.rem(lev + 1, n_lev)),
                    device_id_type=MESH,
                )
            )
            level_down[stage].append(
                pltpu.make_async_remote_copy(
                    src_ref=down_from.at[:, part],
                    dst_ref=down_to.at[:, part],
                    send_sem=lev_send.at[index + 1],
                    recv_sem=lev_recv.at[index + 1],
                    device_id=(me, lax.rem(lev + n_lev - 1, n_lev)),
                    device_id_type=MESH,
                )
            )
            index += 2

    def level_start(stage):
        @pl.when(lev < n_lev - 1)
        def _():
            for copy in level_up[stage]:
                copy.start()

        @pl.when(lev > 0)
        def _():
            for copy in level_down[stage]:
                copy.start()

    def level_wait(stage):
        @pl.when(lev > 0)
        def _():
            for copy in level_up[stage]:
                copy.wait_recv()

        @pl.when(lev < n_lev - 1)
        def _():
            for copy in level_down[stage]:
                copy.wait_recv()

    sends = {
        0: ("e0", "g0w", "g0l"),
        7: ("e7",),
        6: ("e6", "m6", "g7z", "g7a", "g6m", "g6l"),
        1: ("m1", "g1h", "g1l"),
        2: ("m2", "g2h", "g2l"),
        3: ("m3", "g3h", "g3w"),
        5: ("m5", "g5w", "g5l"),
    }
    for position, d in enumerate(SEND_ORDER):
        slotted = slots_of(d)
        weight_copies[d].wait()
        window = lax.dot_general(
            slotted, weight[d], (((1,), (1,)), ((), ())), preferred_element_type=jnp.float32
        )
        if d == centre:
            recv[d] = window
        else:
            outgoing[d] = window
            if position == 0:
                pl.semaphore_wait(
                    barrier,
                    2 * centre + (lev > 0).astype(jnp.int32) + (lev < n_lev - 1).astype(jnp.int32),
                )
            send(*sends[d])
            if position == 0:
                for copy in coef_edges:
                    copy.start()

    @pl.when(parity == 1)
    def _():
        for b in (1, 2, 3):
            arrived(f"m{b}")
            summed[b - 1] = outgoing[b - 1, :, pl.ds(half, half)] + mixing[b - 1]
            forward[f"c{b}"].start()

    @pl.when(parity == 0)
    def _():
        arrived("m6")
        part = pl.ds(0, LANES)
        summed[1, :, part] = outgoing[7, :, part] + mixing[1, :, part]
        forward["c7"].start()
        arrived("m5")
        summed[0] = outgoing[6, :, pl.ds(0, half)] + mixing[0]
        forward["c6"].start()

    def finish(column, width, *pieces):
        value = None
        for d, at in pieces:
            piece = recv[d, :, pl.ds(at, width)]
            value = piece if value is None else value + piece
        for m in range(tracers):
            part = pl.ds(m * levels, levels)
            loss[part, pl.ds(column, width)] = 2.0 * kappa_ref[m] * value[m * levels : (m + 1) * levels]
        delta[:, pl.ds(LANES + column, width)] = value[rows:]

    def level_rows(width):
        return lax.broadcasted_iota(jnp.int32, (levels, width), 0)

    def tangent_partial(lo, hi, tang_to, at, up_to, down_to, out_at):
        width = (hi - lo) * LANES
        own = pl.ds(LANES + lo * LANES, width)
        courant, offset = coef[pl.ds(0, 1), own], coef[pl.ds(1, 1), own]
        rising, sinking = coef[pl.ds(2, 1), own], coef[pl.ds(3, 1), own]
        level = level_rows(width)
        for m in range(tracers):
            part = pl.ds(m * levels, levels)
            wide = delta[part, pl.ds(lo * LANES, width + 2 * LANES)]
            here = wide[:, LANES : LANES + width]
            departed = jnp.zeros_like(here)
            for shift in range(-HALO, HALO + 1):
                moved = here
                if shift != 0:
                    moved = pltpu.roll(wide, (-shift) % (width + 2 * LANES), 1)[:, LANES : LANES + width]
                departed = jnp.where(offset == float(shift), moved, departed)
            below = jnp.where(level == 0, 0.0, pltpu.roll(here, 1, 0))
            above = jnp.where(level == levels - 1, 0.0, pltpu.roll(here, levels - 1, 0))
            value = (
                here
                + courant * (departed - here)
                + rising * (below - here)
                + sinking * (above - here)
                - loss[part, pl.ds(lo * LANES, width)] * here
            )
            tang_to[part, pl.ds(at, width)] = value
            out = pl.ds(out_at, width)
            up_to[pl.ds(m, 1), out] = value[levels - 1 : levels]
            up_to[pl.ds(tracers + m, 1), out] = here[levels - 1 : levels]
            down_to[pl.ds(m, 1), out] = value[0:1]
            down_to[pl.ds(tracers + m, 1), out] = here[0:1]

    def level_terms(value, m, width, rising, sinking, below, above, out):
        level = level_rows(width)
        value = value + jnp.where(level == 0, rising * below[pl.ds(tracers + m, 1), out], 0.0)
        return value + jnp.where(level == levels - 1, sinking * above[pl.ds(tracers + m, 1), out], 0.0)

    def tangent_finish(lo, hi):
        width = (hi - lo) * LANES
        own = pl.ds(LANES + lo * LANES, width)
        out = pl.ds(lo * LANES, width)
        rising, sinking = coef[pl.ds(2, 1), own], coef[pl.ds(3, 1), own]
        for m in range(tracers):
            part = pl.ds(m * levels, levels)
            value = level_terms(tang[part, own], m, width, rising, sinking, below_in, above_in, out)
            tang[part, own] = value
            tangent_out[m, :, out] = value

    def main_partial(ranges):
        for lo, hi in ranges:
            tangent_partial(lo, hi, tang, LANES + lo * LANES, up_out, down_out, lo * LANES)

    def adjoint(lo, hi):
        width = (hi - lo) * LANES
        own = pl.ds(LANES + lo * LANES, width)
        out = pl.ds(lo * LANES, width)
        around = pl.ds(lo * LANES, width + 2 * LANES)
        courant, rising, sinking = coef[pl.ds(0, 1), own], coef[pl.ds(2, 1), own], coef[pl.ds(3, 1), own]
        wide_courant, wide_offset = coef[pl.ds(0, 1), around], coef[pl.ds(1, 1), around]
        level = level_rows(width)
        pieces = []
        for m in range(tracers):
            part = pl.ds(m * levels, levels)
            wide = tang[part, around]
            here = wide[:, LANES : LANES + width]
            total = jnp.zeros_like(here)
            for shift in range(-HALO, HALO + 1):
                term = jnp.where(wide_offset == float(shift), wide_courant, 0.0) * wide
                if shift != 0:
                    term = pltpu.roll(term, shift % (width + 2 * LANES), 1)
                total = total + term[:, LANES : LANES + width]
            own_delta = delta[part, own]
            under = below_in[pl.ds(m, 1), out] + sinking * own_delta[0:1]
            over = above_in[pl.ds(m, 1), out] + rising * own_delta[levels - 1 : levels]
            under = jnp.where(lev > 0, under, 0.0)
            over = jnp.where(lev < n_lev - 1, over, 0.0)
            lower = jnp.where(level == 0, under, pltpu.roll(here, 1, 0))
            upper = jnp.where(level == levels - 1, over, pltpu.roll(here, levels - 1, 0))
            diagonal = 1.0 - courant - rising - sinking - loss[part, out]
            pieces.append(diagonal * here + total + rising * upper + sinking * lower)
        value = jnp.concatenate(pieces, axis=0).astype(jnp.bfloat16)
        adj[:, out] = value
        if lo == 0:
            adj[:, pl.ds(cols, span)] = value[:, :span]

    last = cols - LANES
    arrived("e0", "e7", "e6")
    finish(0, LANES, (0, 0), (7, half))
    finish(last, LANES, (7, LANES), (6, 3 * LANES))
    for copy in delta_edges:
        copy.start()
    for d in (0, 7, 6):
        place_weight(d)
    for copy in (*delta_edges, *coef_edges):
        copy.wait_recv()
    tangent_partial(tiles - 1, tiles, edge_tang, 0, edge_up, edge_down, 0)
    tangent_partial(0, 1, edge_tang, LANES, edge_up, edge_down, LANES)
    level_start(0)
    for d in (1, 2, 3):
        place_weight(d)
    level_wait(0)
    for at, tile in ((0, tiles - 1), (LANES, 0)):
        own = pl.ds(LANES + tile * LANES, LANES)
        out = pl.ds(at, LANES)
        for m in range(tracers):
            part = pl.ds(m * levels, levels)
            edge_tang[part, out] = level_terms(
                edge_tang[part, out], m, LANES, coef[pl.ds(2, 1), own], coef[pl.ds(3, 1), own], edge_below, edge_above, out
            )
    for copy in tang_edges:
        copy.start()
    for d in (5, 4):
        place_weight(d)

    arrived("g7z")

    @pl.when(parity == 0)
    def _():
        arrived("g0w", "g7a", "g6m", "g5l", "g1l", "c6", "c2")
        finish(LANES, LANES, (0, LANES), (7, 3 * LANES))
        finish(last - LANES, LANES, (7, 0), (6, half))
        finish(span, span, (1, 0), (0, half))
        finish(2 * span, span, (2, 0))
        finish(5 * span, span, (5, 0), (4, half))
        finish(6 * span, span, (6, 0))

    @pl.when(parity == 1)
    def _():
        arrived("g0l", "c7", "g6l", "g5w", "g2l", "g1h", "c1")
        finish(LANES, LANES, (0, LANES), (7, 3 * LANES))
        finish(last - LANES, LANES, (7, 0))
        finish(span, span, (1, 0))
        finish(2 * span, span, (2, 0), (1, half))
        finish(5 * span, span, (5, 0), (4, half))
        finish(6 * span, span, (6, 0), (5, half))

    main_partial(early)
    level_start(1)

    @pl.when(parity == 0)
    def _():
        arrived("g2h", "g3w")
        finish(3 * span, span, (3, 0), (2, half))
        finish(4 * span, span, (4, 0), (3, half))

    @pl.when(parity == 1)
    def _():
        arrived("c3", "g3h")
        finish(3 * span, span, (3, 0))
        finish(4 * span, span, (4, 0), (3, half))

    main_partial(late)
    level_start(2)
    level_wait(1)
    for lo, hi in early:
        tangent_finish(lo, hi)
    for copy in tang_edges:
        copy.wait_recv()
    adjoint(0, 4)
    adjoint(12, tiles)
    for d in (0, 7, 6):
        giving[d].start()
    level_wait(2)
    for lo, hi in late:
        tangent_finish(lo, hi)
    adjoint(4, 12)
    for d in (1, 2, 5, 3):
        giving[d].start()

    for d in (centre, 0, 7, 6, 1, 2, 5, 3):
        if d == centre:
            returned = adj[:, pl.ds(d * span, win)]
        else:
            giving[d].wait_recv()
            returned = back[d]
        grad = jnp.dot(returned, shifted[d], preferred_element_type=jnp.float32)
        for t in range(parts + 1):
            placed[d, t + 1] = grad[:, t * LANES : (t + 1) * LANES]

    top = placed.shape[1] - 1
    for t in range(tiles):
        value = None
        for d in range(reach):
            at = lax.min(lax.max(t + 1 - firsts[d], 0), top)
            piece = placed[d, at]
            value = piece if value is None else value + piece
        for m in range(tracers):
            grad_out[m, :, pl.ds(t * LANES, LANES)] = value[m * levels : (m + 1) * levels]

    for name, copy in forward.items():
        on_core(plan[name][0], copy.wait_send)
    for copy in (*giving.values(), *coef_edges, *delta_edges, *tang_edges):
        copy.wait_send()

    @pl.when(lev < n_lev - 1)
    def _():
        for copies in level_up:
            for copy in copies:
                copy.wait_send()

    @pl.when(lev > 0)
    def _():
        for copies in level_down:
            for copy in copies:
                copy.wait_send()


def shards(n_tile, n_lev, trajectory, increment, counts, remap_weight, kappa, courant, vertical, offset):
    tracers, levels, cols = trajectory.shape
    reach, win, cap = remap_weight.shape[1:]
    rows = tracers * levels
    span = cols // reach
    wide = cols + 2 * LANES
    f32, bf16 = jnp.float32, jnp.bfloat16
    vmem = pl.BlockSpec(memory_space=pltpu.VMEM)
    dma = pltpu.SemaphoreType.DMA
    out = jax.ShapeDtypeStruct((tracers, levels, cols), f32)
    return pl.pallas_call(
        functools.partial(kernel, n_tile, n_lev),
        out_shape=(out, out),
        in_specs=[pl.BlockSpec(memory_space=pltpu.HBM)] * 8,
        out_specs=(vmem, vmem),
        scratch_shapes=[
            pltpu.VMEM((tracers, levels, cols), bf16),
            pltpu.VMEM((tracers, levels, cols), bf16),
            pltpu.SMEM((1, reach), jnp.int32),
            pltpu.SMEM((tracers,), f32),
            pltpu.VMEM((1, cols), f32),
            pltpu.VMEM((1, cols), f32),
            pltpu.VMEM((1, cols), jnp.int32),
            pltpu.VMEM((reach, win, cap), bf16),
            pltpu.VMEM((reach, win, cap + LANES), bf16),
            pltpu.VMEM((cols // LANES + cap // LANES + 1, 2 * rows, LANES), bf16),
            pltpu.VMEM((reach, 2 * rows, win), f32),
            pltpu.VMEM((3, 2 * rows, win // 2), f32),
            pltpu.VMEM((3, 2 * rows, win // 2), f32),
            pltpu.VMEM((reach, 2 * rows, win), f32),
            pltpu.VMEM((8, wide), f32),
            pltpu.VMEM((rows, wide), f32),
            pltpu.VMEM((rows, cols), f32),
            pltpu.VMEM((rows, wide), f32),
            pltpu.VMEM((8, cols), f32),
            pltpu.VMEM((8, cols), f32),
            pltpu.VMEM((8, cols), f32),
            pltpu.VMEM((8, cols), f32),
            pltpu.VMEM((8, 2 * LANES), f32),
            pltpu.VMEM((8, 2 * LANES), f32),
            pltpu.VMEM((8, 2 * LANES), f32),
            pltpu.VMEM((8, 2 * LANES), f32),
            pltpu.VMEM((rows, 2 * LANES), f32),
            pltpu.VMEM((rows, cols + span), bf16),
            pltpu.VMEM((reach, rows, win), bf16),
            pltpu.VMEM((reach, cap // LANES + 3, rows, LANES), f32),
            dma((7,)),
            dma((reach,)),
            dma((27,)),
            dma((27,)),
            dma((2,)),
            dma((2,)),
            dma((4,)),
            dma((4,)),
            dma((10,)),
            dma((10,)),
            dma((reach,)),
            dma((reach,)),
        ],
        compiler_params=pltpu.CompilerParams(
            collective_id=0, has_side_effects=True, vmem_limit_bytes=24 * 1024 * 1024
        ),
    )(
        *(
            pltpu.with_memory_space_constraint(operand, pltpu.HBM)
            for operand in (
                trajectory,
                increment,
                counts,
                kappa,
                courant.reshape(1, cols),
                vertical.reshape(1, cols),
                offset.reshape(1, cols),
                remap_weight,
            )
        )
    )


def solution(mesh):
    return jax.shard_map(
        functools.partial(shards, mesh.shape["tile"], mesh.shape["lev"]),
        mesh=mesh,
        in_specs=(
            P(None, "lev", "tile"),
            P(None, "lev", "tile"),
            P("tile", None),
            P("tile", None, None, None),
            P(),
            P("tile"),
            P("tile"),
            P("tile"),
        ),
        out_specs=(P(None, "lev", "tile"), P(None, "lev", "tile")),
        check_vma=False,
    )
```

```python
import functools

import jax
import jax.numpy as jnp
from jax import lax
from jax.experimental import pallas as pl
from jax.experimental.pallas import tpu as pltpu
from jax.sharding import PartitionSpec as P

MESH = pl.DeviceIdType.MESH
LANES = 128
HALO = 2
FIRST, REST = (0, 7, 6), (1, 2, 3, 5, 4)
EVEN, ODD = (0,), (1,)
BOTH = (0, 1)


def kernel(
    n_tile,
    n_lev,
    traj_hbm,
    inc_hbm,
    counts_hbm,
    kappa_hbm,
    courant_hbm,
    vertical_hbm,
    offset_hbm,
    weight_hbm,
    tangent_out,
    grad_out,
    traj_ref,
    inc_ref,
    counts_ref,
    kappa_ref,
    courant_ref,
    vertical_ref,
    offset_ref,
    weight,
    shifted,
    fields,
    outgoing,
    mixing,
    summed,
    recv,
    coef,
    delta,
    loss,
    tang,
    up_out,
    down_out,
    below_in,
    above_in,
    tiny_out,
    tiny_in,
    turn,
    adj,
    back,
    placed,
    load_sem,
    weight_sem,
    fwd_send,
    fwd_recv,
    coef_send,
    coef_recv,
    tiny_send,
    tiny_recv,
    lev_send,
    lev_recv,
    ret_recv,
):
    tracers, levels, cols = traj_hbm.shape
    rows = tracers * levels
    reach = weight_hbm.shape[1]
    win, cap = weight_hbm.shape[2], weight_hbm.shape[3]
    centre = reach // 2
    span = cols // reach
    tiles = cols // LANES
    sub = span // LANES
    me = lax.axis_index("tile")
    lev = lax.axis_index("lev")

    def tile_at(distance):
        return (lax.rem(me + (n_tile + distance), n_tile), lev)

    barrier = pltpu.get_barrier_semaphore()
    radius = centre + 1
    for distance in range(-radius, radius + 1):
        if distance != 0:
            pl.semaphore_signal(barrier, inc=1, device_id=tile_at(distance), device_id_type=MESH)

    @pl.when(lev > 0)
    def _():
        pl.semaphore_signal(barrier, inc=1, device_id=(me, lev - 1), device_id_type=MESH)

    @pl.when(lev < n_lev - 1)
    def _():
        pl.semaphore_signal(barrier, inc=1, device_id=(me, lev + 1), device_id_type=MESH)

    loads = [
        pltpu.make_async_copy(source, target, load_sem.at[i])
        for i, (source, target) in enumerate(
            (
                (counts_hbm, counts_ref),
                (kappa_hbm, kappa_ref),
                (traj_hbm, traj_ref),
                (inc_hbm, inc_ref),
                (courant_hbm, courant_ref),
                (vertical_hbm, vertical_ref),
                (offset_hbm, offset_ref),
            )
        )
    ]
    weight_copies = {
        d: pltpu.make_async_copy(weight_hbm.at[0, d], weight.at[d], sem)
        for group, sems in ((FIRST, weight_sem), (REST, load_sem))
        for d, sem in ((d, sems.at[i]) for i, d in enumerate(group))
    }
    for copy in loads:
        copy.start()
    for d in FIRST:
        weight_copies[d].start()

    for copy in loads:
        copy.wait()
    for d in REST:
        weight_copies[d].start()
    stacked = jnp.concatenate(
        [ref[m].astype(jnp.float32) for ref in (traj_ref, inc_ref) for m in range(tracers)], axis=0
    ).astype(jnp.bfloat16)
    for t in range(tiles):
        fields[t] = stacked[:, t * LANES : (t + 1) * LANES]
    for t in range(tiles, fields.shape[0]):
        fields[t] = jnp.zeros((2 * rows, LANES), jnp.bfloat16)
    vertical = vertical_ref[...]
    coef[pl.ds(0, 1), pl.ds(LANES, cols)] = courant_ref[...]
    coef[pl.ds(1, 1), pl.ds(LANES, cols)] = offset_ref[...].astype(jnp.float32)
    coef[pl.ds(2, 1), pl.ds(LANES, cols)] = jnp.maximum(vertical, 0.0)
    coef[pl.ds(3, 1), pl.ds(LANES, cols)] = jnp.maximum(-vertical, 0.0)
    coef[pl.ds(4, 4), pl.ds(LANES, cols)] = jnp.zeros((4, cols), jnp.float32)
    for ref in (up_out, down_out):
        ref[pl.ds(6, 2), :] = jnp.zeros((2, ref.shape[1]), jnp.float32)
    turn[...] = jnp.zeros_like(turn)
    for at in (0, delta.shape[1] - LANES):
        delta[:, pl.ds(at, LANES)] = jnp.zeros((rows, LANES), jnp.float32)

    @pl.when(lev == 0)
    def _():
        below_in[...] = jnp.zeros_like(below_in)

    @pl.when(lev == n_lev - 1)
    def _():
        above_in[...] = jnp.zeros_like(above_in)

    placed[:, pl.ds(0, 1)] = jnp.zeros((reach, 1, rows, LANES), jnp.float32)
    placed[:, pl.ds(placed.shape[1] - 1, 1)] = jnp.zeros((reach, 1, rows, LANES), jnp.float32)

    starts = []
    total = jnp.int32(0)
    for d in range(reach):
        starts.append(total)
        total = total + counts_ref[0, d]

    firsts = [lax.shift_right_logical(start, 7) for start in starts]
    shifts = [lax.bitwise_and(start, LANES - 1) for start in starts]
    parts = cap // LANES
    lane = lax.broadcasted_iota(jnp.int32, (2 * rows, LANES), 1)
    skew = lax.broadcasted_iota(jnp.int32, (2 * LANES, LANES), 0) - lax.broadcasted_iota(
        jnp.int32, (2 * LANES, LANES), 1
    )

    def selection(amount):
        return jnp.where(skew == amount, 1.0, 0.0).astype(jnp.bfloat16)

    def slots_of(d):
        loaded = [fields[firsts[d] + t] for t in range(parts + 1)]
        pairs = [jnp.concatenate([loaded[t], loaded[t + 1]], axis=1) for t in range(parts)]
        moved = jnp.dot(
            jnp.concatenate(pairs, axis=0), selection(shifts[d]), preferred_element_type=jnp.float32
        )
        pieces = []
        for t in range(parts):
            value = moved[t * 2 * rows : (t + 1) * 2 * rows]
            pieces.append(jnp.where(lane + t * LANES < counts_ref[0, d], value, 0.0).astype(jnp.bfloat16))
        return jnp.concatenate(pieces, axis=1)

    tall = lax.broadcasted_iota(jnp.int32, (win, LANES), 1)

    def place_weight(d):
        chosen = selection(LANES - shifts[d])
        nothing = jnp.zeros((win, LANES), jnp.bfloat16)
        live = []
        for t in range(parts):
            piece = weight[d, :, pl.ds(t * LANES, LANES)]
            live.append(jnp.where(tall + t * LANES < counts_ref[0, d], piece, nothing))
        live = [nothing, *live, nothing]
        for t in range(parts + 1):
            moved = jnp.dot(
                jnp.concatenate([live[t], live[t + 1]], axis=1), chosen, preferred_element_type=jnp.float32
            )
            shifted[d, :, pl.ds(t * LANES, LANES)] = moved.astype(jnp.bfloat16)

    parity = lax.rem(me, 2)
    half = win // 2

    def on_core(cores, run):
        if len(cores) == 2:
            run()
        else:
            pl.when(parity == cores[0])(run)

    def window_part(d, lane, width):
        part = pl.ds(lane, width)
        return outgoing.at[d, :, part], recv.at[d, :, part], d - centre

    plan = {
        "g0w": (EVEN, 0, 0, *window_part(0, 0, win)),
        "g0l": (ODD, 0, 0, *window_part(0, 0, half)),
        "g1h": (EVEN, 1, 1, *window_part(1, half, half)),
        "g1l": (ODD, 1, 1, *window_part(1, 0, half)),
        "g2h": (EVEN, 2, 2, *window_part(2, half, half)),
        "g2l": (ODD, 2, 2, *window_part(2, 0, half)),
        "g3h": (EVEN, 3, 3, *window_part(3, half, half)),
        "g3w": (ODD, 3, 3, *window_part(3, 0, win)),
        "g5w": (EVEN, 4, 4, *window_part(5, 0, win)),
        "g5l": (ODD, 4, 4, *window_part(5, 0, half)),
        "g6h": (EVEN, 5, 5, *window_part(6, half, half)),
        "g6l": (ODD, 5, 5, *window_part(6, 0, half)),
        "g7h": (EVEN, 6, 6, *window_part(7, half, half)),
        "g7w": (ODD, 6, 6, *window_part(7, 0, win)),
        "m1": (EVEN, 7, 10, outgoing.at[1, :, pl.ds(0, half)], mixing.at[0], 1),
        "m2": (EVEN, 8, 11, outgoing.at[2, :, pl.ds(0, half)], mixing.at[1], 1),
        "m3": (EVEN, 9, 12, outgoing.at[3, :, pl.ds(0, half)], mixing.at[2], 1),
        "m5": (ODD, 7, 10, outgoing.at[5, :, pl.ds(half, half)], mixing.at[0], -1),
        "m6": (ODD, 8, 11, outgoing.at[6, :, pl.ds(half, half)], mixing.at[1], -1),
        "c1": (ODD, 9, 7, summed.at[0], recv.at[1, :, pl.ds(0, half)], -4),
        "c2": (ODD, 10, 7, summed.at[1], recv.at[2, :, pl.ds(0, half)], -3),
        "c3": (ODD, 11, 8, summed.at[2], recv.at[3, :, pl.ds(0, half)], -2),
        "c6": (EVEN, 10, 8, summed.at[0], recv.at[6, :, pl.ds(0, half)], 2),
        "c7": (EVEN, 11, 9, summed.at[1], recv.at[7, :, pl.ds(0, half)], 3),
    }
    forward = {
        name: pltpu.make_async_remote_copy(
            src_ref=source,
            dst_ref=target,
            send_sem=fwd_send.at[leaving],
            recv_sem=fwd_recv.at[landing],
            device_id=tile_at(distance),
            device_id_type=MESH,
        )
        for name, (_, leaving, landing, source, target, distance) in plan.items()
    }
    corners = ((0, 0, 0, -5), (7, half, 0, 2), (7, half - 16, 8, 4), (6, win - 16, 8, 3))
    halo_parts = [
        pltpu.make_async_remote_copy(
            src_ref=tiny_out.at[i],
            dst_ref=tiny_in.at[i],
            send_sem=tiny_send.at[i],
            recv_sem=tiny_recv.at[i],
            device_id=tile_at(distance),
            device_id_type=MESH,
        )
        for i, (_, _, _, distance) in enumerate(corners)
    ]

    def send(*names):
        for name in names:
            on_core(plan[name][0], forward[name].start)

    def arrived(*names):
        for name in names:
            forward[name].wait_recv()

    giving = {
        d: pltpu.make_async_remote_copy(
            src_ref=adj.at[:, pl.ds(d * span, win)],
            dst_ref=back.at[d],
            send_sem=fwd_send.at[d if d < centre else d - 1],
            recv_sem=ret_recv.at[d],
            device_id=tile_at(centre - d),
            device_id_type=MESH,
        )
        for d in range(reach)
        if d != centre
    }

    coef_edges = [
        pltpu.make_async_remote_copy(
            src_ref=coef.at[:, pl.ds(source, LANES)],
            dst_ref=coef.at[:, pl.ds(target, LANES)],
            send_sem=coef_send.at[i],
            recv_sem=coef_recv.at[i],
            device_id=tile_at(distance),
            device_id_type=MESH,
        )
        for i, (source, target, distance) in enumerate(((LANES, LANES + cols, -1), (cols, 0, 1)))
    ]

    early = ((-1, 1), (11, tiles + 1))
    middle = ((1, 5),)
    late = ((5, 11),)
    level_up, level_down = ([], [], []), ([], [], [])
    index = 0
    for stage, ranges in enumerate((early, middle, late)):
        for lo, hi in ranges:
            part = pl.ds((lo + 1) * LANES, (hi - lo) * LANES)
            for ways, source, target, distance in (
                (level_up, up_out, below_in, 1),
                (level_down, down_out, above_in, n_lev - 1),
            ):
                ways[stage].append(
                    pltpu.make_async_remote_copy(
                        src_ref=source.at[:, part],
                        dst_ref=target.at[:, part],
                        send_sem=lev_send.at[index],
                        recv_sem=lev_recv.at[index],
                        device_id=(me, lax.rem(lev + distance, n_lev)),
                        device_id_type=MESH,
                    )
                )
                index += 1

    def level_start(stage):
        @pl.when(lev < n_lev - 1)
        def _():
            for copy in level_up[stage]:
                copy.start()

        @pl.when(lev > 0)
        def _():
            for copy in level_down[stage]:
                copy.start()

    def level_wait(stage):
        @pl.when(lev > 0)
        def _():
            for copy in level_up[stage]:
                copy.wait_recv()

        @pl.when(lev < n_lev - 1)
        def _():
            for copy in level_down[stage]:
                copy.wait_recv()

    sends = {
        0: ("g0w", "g0l"),
        7: ("g7h", "g7w"),
        6: ("m6", "g6h", "g6l"),
        1: ("m1", "g1h", "g1l"),
        2: ("m2", "g2h", "g2l"),
        3: ("m3", "g3h", "g3w"),
        5: ("m5", "g5w", "g5l"),
    }

    def windows(groups):
        slotted = {d: slots_of(d) for d in groups}
        for d in groups:
            weight_copies[d].wait()
        for i, (d, column, row, _) in enumerate(corners):
            if d in groups:
                corner = lax.dot_general(
                    weight[d, pl.ds(column, 16), :],
                    slotted[d],
                    (((1,), (1,)), ((), ())),
                    preferred_element_type=jnp.float32,
                )
                tiny_out[i, :, pl.ds(0, 2 * rows)] = corner[row : row + 8]
        for d in groups:
            window = lax.dot_general(
                slotted[d], weight[d], (((1,), (1,)), ((), ())), preferred_element_type=jnp.float32
            )
            if d == centre:
                recv[d] = window
            else:
                outgoing[d] = window

    tiny_out[...] = jnp.zeros_like(tiny_out)
    windows(FIRST)
    pl.semaphore_wait(
        barrier, 2 * radius + (lev > 0).astype(jnp.int32) + (lev < n_lev - 1).astype(jnp.int32)
    )
    for copy in (*halo_parts, *coef_edges):
        copy.start()
    for d in FIRST:
        send(*sends[d])
    windows(REST)
    for d in REST:
        if d != centre:
            send(*sends[d])
    for d in FIRST:
        place_weight(d)

    @pl.when(parity == 1)
    def _():
        for b in (1, 2, 3):
            arrived(f"m{b}")
            summed[b - 1] = outgoing[b - 1, :, pl.ds(half, half)] + mixing[b - 1]
            forward[f"c{b}"].start()

    @pl.when(parity == 0)
    def _():
        arrived("m6")
        summed[1] = outgoing[7, :, pl.ds(0, half)] + mixing[1]
        forward["c7"].start()
        arrived("m5")
        summed[0] = outgoing[6, :, pl.ds(0, half)] + mixing[0]
        forward["c6"].start()

    def finish(column, width, *pieces):
        value = None
        for d, at in pieces:
            piece = recv[d, :, pl.ds(at, width)]
            value = piece if value is None else value + piece
        for m in range(tracers):
            part = pl.ds(m * levels, levels)
            loss[part, pl.ds(LANES + column, width)] = 2.0 * kappa_ref[m] * value[m * levels : (m + 1) * levels]
        delta[:, pl.ds(2 * LANES + column, width)] = value[rows:]

    def finish_halo():
        turn[pl.ds(0, 8), :] = tiny_in[0] + tiny_in[1]
        turn[pl.ds(LANES - 8, 8), :] = tiny_in[2] + tiny_in[3]
        value = jnp.transpose(turn[...])
        for at in (0, LANES + cols):
            for m in range(tracers):
                part = pl.ds(m * levels, levels)
                loss[part, pl.ds(at, LANES)] = 2.0 * kappa_ref[m] * value[m * levels : (m + 1) * levels]
            delta[:, pl.ds(LANES + at, LANES)] = value[rows : 2 * rows]

    def level_rows(width):
        return lax.broadcasted_iota(jnp.int32, (levels, width), 0)

    def tangent_partial(lo, hi):
        width = (hi - lo) * LANES
        own = pl.ds(LANES + lo * LANES, width)
        courant, offset = coef[pl.ds(0, 1), own], coef[pl.ds(1, 1), own]
        rising, sinking = coef[pl.ds(2, 1), own], coef[pl.ds(3, 1), own]
        level = level_rows(width)
        for m in range(tracers):
            part = pl.ds(m * levels, levels)
            wide = delta[part, pl.ds((lo + 1) * LANES, width + 2 * LANES)]
            here = wide[:, LANES : LANES + width]
            departed = jnp.zeros_like(here)
            for shift in range(-HALO, HALO + 1):
                moved = here
                if shift != 0:
                    moved = pltpu.roll(wide, (-shift) % (width + 2 * LANES), 1)[:, LANES : LANES + width]
                departed = jnp.where(offset == float(shift), moved, departed)
            below = jnp.where(level == 0, 0.0, pltpu.roll(here, 1, 0))
            above = jnp.where(level == levels - 1, 0.0, pltpu.roll(here, levels - 1, 0))
            value = (
                here
                + courant * (departed - here)
                + rising * (below - here)
                + sinking * (above - here)
                - loss[part, own] * here
            )
            tang[part, own] = value
            up_out[pl.ds(m, 1), own] = value[levels - 1 : levels]
            up_out[pl.ds(tracers + m, 1), own] = here[levels - 1 : levels]
            down_out[pl.ds(m, 1), own] = value[0:1]
            down_out[pl.ds(tracers + m, 1), own] = here[0:1]

    def tangent_finish(lo, hi):
        width = (hi - lo) * LANES
        own = pl.ds(LANES + lo * LANES, width)
        rising, sinking = coef[pl.ds(2, 1), own], coef[pl.ds(3, 1), own]
        level = level_rows(width)
        inner_lo, inner_hi = max(lo, 0), min(hi, tiles)
        for m in range(tracers):
            part = pl.ds(m * levels, levels)
            value = tang[part, own]
            value = value + jnp.where(level == 0, rising * below_in[pl.ds(tracers + m, 1), own], 0.0)
            value = value + jnp.where(level == levels - 1, sinking * above_in[pl.ds(tracers + m, 1), own], 0.0)
            tang[part, own] = value
            tangent_out[m, :, pl.ds(inner_lo * LANES, (inner_hi - inner_lo) * LANES)] = value[
                :, (inner_lo - lo) * LANES : (inner_hi - lo) * LANES
            ]

    def adjoint(lo, hi):
        width = (hi - lo) * LANES
        own = pl.ds(LANES + lo * LANES, width)
        out = pl.ds(lo * LANES, width)
        around = pl.ds(lo * LANES, width + 2 * LANES)
        courant, rising, sinking = coef[pl.ds(0, 1), own], coef[pl.ds(2, 1), own], coef[pl.ds(3, 1), own]
        wide_courant, wide_offset = coef[pl.ds(0, 1), around], coef[pl.ds(1, 1), around]
        level = level_rows(width)
        pieces = []
        for m in range(tracers):
            part = pl.ds(m * levels, levels)
            wide = tang[part, around]
            here = wide[:, LANES : LANES + width]
            total = jnp.zeros_like(here)
            for shift in range(-HALO, HALO + 1):
                term = jnp.where(wide_offset == float(shift), wide_courant, 0.0) * wide
                if shift != 0:
                    term = pltpu.roll(term, shift % (width + 2 * LANES), 1)
                total = total + term[:, LANES : LANES + width]
            own_delta = delta[part, pl.ds((lo + 2) * LANES, width)]
            under = below_in[pl.ds(m, 1), own] + sinking * own_delta[0:1]
            over = above_in[pl.ds(m, 1), own] + rising * own_delta[levels - 1 : levels]
            under = jnp.where(lev > 0, under, 0.0)
            over = jnp.where(lev < n_lev - 1, over, 0.0)
            lower = jnp.where(level == 0, under, pltpu.roll(here, 1, 0))
            upper = jnp.where(level == levels - 1, over, pltpu.roll(here, levels - 1, 0))
            diagonal = 1.0 - courant - rising - sinking - loss[part, own]
            pieces.append(diagonal * here + total + rising * upper + sinking * lower)
        value = jnp.concatenate(pieces, axis=0).astype(jnp.bfloat16)
        adj[:, out] = value
        if lo == 0:
            adj[:, pl.ds(cols, span)] = value[:, :span]

    for d in REST:
        place_weight(d)
    for copy in (*halo_parts, *coef_edges):
        copy.wait_recv()
    finish_halo()

    @pl.when(parity == 0)
    def _():
        arrived("g0w", "g7w", "g6h", "g5l", "c6")
        finish(0, span, (0, 0), (7, half))
        finish(7 * span, span, (7, 0), (6, half))
        finish(5 * span, span, (5, 0), (4, half))
        finish(6 * span, span, (6, 0))

    @pl.when(parity == 1)
    def _():
        arrived("g0l", "g7h", "c7", "g6l", "g5w")
        finish(0, span, (0, 0), (7, half))
        finish(7 * span, span, (7, 0))
        finish(5 * span, span, (5, 0), (4, half))
        finish(6 * span, span, (6, 0), (5, half))

    for lo, hi in early:
        tangent_partial(lo, hi)
    level_start(0)

    @pl.when(parity == 0)
    def _():
        arrived("g1l", "c2")
        finish(span, span, (1, 0), (0, half))
        finish(2 * span, span, (2, 0))

    @pl.when(parity == 1)
    def _():
        arrived("c1", "g2l", "g1h")
        finish(span, span, (1, 0))
        finish(2 * span, span, (2, 0), (1, half))

    for lo, hi in middle:
        tangent_partial(lo, hi)
    level_start(1)

    @pl.when(parity == 0)
    def _():
        arrived("g2h", "g3w")
        finish(3 * span, span, (3, 0), (2, half))
        finish(4 * span, span, (4, 0), (3, half))

    @pl.when(parity == 1)
    def _():
        arrived("g3h", "c3")
        finish(3 * span, span, (3, 0))
        finish(4 * span, span, (4, 0), (3, half))

    for lo, hi in late:
        tangent_partial(lo, hi)
    level_start(2)
    level_wait(0)
    for lo, hi in early:
        tangent_finish(lo, hi)
    level_wait(1)
    for lo, hi in middle:
        tangent_finish(lo, hi)
    adjoint(0, 4)
    adjoint(12, tiles)
    for name, copy in forward.items():
        on_core(plan[name][0], copy.wait_send)
    for d in (0, 7, 6):
        giving[d].start()
    level_wait(2)
    for lo, hi in late:
        tangent_finish(lo, hi)
    adjoint(4, 12)
    for d in (1, 2, 5, 3):
        giving[d].start()

    def grads(groups):
        for d in groups:
            if d != centre:
                giving[d].wait_recv()
        for d in groups:
            returned = adj[:, pl.ds(d * span, win)] if d == centre else back[d]
            grad = jnp.dot(returned, shifted[d], preferred_element_type=jnp.float32)
            for t in range(parts + 1):
                placed[d, t + 1] = grad[:, t * LANES : (t + 1) * LANES]

    grads((centre, 0, 7, 6))
    grads((1, 2, 5, 3))

    top = placed.shape[1] - 1
    for t in range(tiles):
        value = None
        for d in range(reach):
            at = lax.min(lax.max(t + 1 - firsts[d], 0), top)
            piece = placed[d, at]
            value = piece if value is None else value + piece
        for m in range(tracers):
            grad_out[m, :, pl.ds(t * LANES, LANES)] = value[m * levels : (m + 1) * levels]

    for copy in (*giving.values(), *coef_edges, *halo_parts):
        copy.wait_send()

    @pl.when(lev < n_lev - 1)
    def _():
        for copies in level_up:
            for copy in copies:
                copy.wait_send()

    @pl.when(lev > 0)
    def _():
        for copies in level_down:
            for copy in copies:
                copy.wait_send()


def shards(n_tile, n_lev, trajectory, increment, counts, remap_weight, kappa, courant, vertical, offset):
    tracers, levels, cols = trajectory.shape
    reach, win, cap = remap_weight.shape[1:]
    rows = tracers * levels
    span = cols // reach
    wide = cols + 2 * LANES
    f32, bf16 = jnp.float32, jnp.bfloat16
    vmem = pl.BlockSpec(memory_space=pltpu.VMEM)
    dma = pltpu.SemaphoreType.DMA
    out = jax.ShapeDtypeStruct((tracers, levels, cols), f32)
    return pl.pallas_call(
        functools.partial(kernel, n_tile, n_lev),
        out_shape=(out, out),
        in_specs=[pl.BlockSpec(memory_space=pltpu.HBM)] * 8,
        out_specs=(vmem, vmem),
        scratch_shapes=[
            pltpu.VMEM((tracers, levels, cols), bf16),
            pltpu.VMEM((tracers, levels, cols), bf16),
            pltpu.SMEM((1, reach), jnp.int32),
            pltpu.SMEM((tracers,), f32),
            pltpu.VMEM((1, cols), f32),
            pltpu.VMEM((1, cols), f32),
            pltpu.VMEM((1, cols), jnp.int32),
            pltpu.VMEM((reach, win, cap), bf16),
            pltpu.VMEM((reach, win, cap + LANES), bf16),
            pltpu.VMEM((cols // LANES + cap // LANES + 1, 2 * rows, LANES), bf16),
            pltpu.VMEM((reach, 2 * rows, win), f32),
            pltpu.VMEM((3, 2 * rows, win // 2), f32),
            pltpu.VMEM((3, 2 * rows, win // 2), f32),
            pltpu.VMEM((reach, 2 * rows, win), f32),
            pltpu.VMEM((8, wide), f32),
            pltpu.VMEM((rows, wide + 2 * LANES), f32),
            pltpu.VMEM((rows, wide), f32),
            pltpu.VMEM((rows, wide), f32),
            pltpu.VMEM((8, wide), f32),
            pltpu.VMEM((8, wide), f32),
            pltpu.VMEM((8, wide), f32),
            pltpu.VMEM((8, wide), f32),
            pltpu.VMEM((4, 8, LANES), f32),
            pltpu.VMEM((4, 8, LANES), f32),
            pltpu.VMEM((LANES, LANES), f32),
            pltpu.VMEM((rows, cols + span), bf16),
            pltpu.VMEM((reach, rows, win), bf16),
            pltpu.VMEM((reach, cap // LANES + 3, rows, LANES), f32),
            dma((7,)),
            dma((len(FIRST),)),
            dma((12,)),
            dma((13,)),
            dma((2,)),
            dma((2,)),
            dma((4,)),
            dma((4,)),
            dma((8,)),
            dma((8,)),
            dma((reach,)),
        ],
        compiler_params=pltpu.CompilerParams(
            collective_id=0, has_side_effects=True, vmem_limit_bytes=24 * 1024 * 1024
        ),
    )(
        *(
            pltpu.with_memory_space_constraint(operand, pltpu.HBM)
            for operand in (
                trajectory,
                increment,
                counts,
                kappa,
                courant.reshape(1, cols),
                vertical.reshape(1, cols),
                offset.reshape(1, cols),
                remap_weight,
            )
        )
    )


def solution(mesh):
    return jax.shard_map(
        functools.partial(shards, mesh.shape["tile"], mesh.shape["lev"]),
        mesh=mesh,
        in_specs=(
            P(None, "lev", "tile"),
            P(None, "lev", "tile"),
            P("tile", None),
            P("tile", None, None, None),
            P(),
            P("tile"),
            P("tile"),
            P("tile"),
        ),
        out_specs=(P(None, "lev", "tile"), P(None, "lev", "tile")),
        check_vma=False,
    )
```

```python
import functools

import jax
import jax.numpy as jnp
from jax import lax
from jax.experimental import pallas as pl
from jax.experimental.pallas import tpu as pltpu
from jax.sharding import PartitionSpec as P

MESH = pl.DeviceIdType.MESH
LANES = 128
HALO = 2
FIRST, SECOND, THIRD = (0,), (1, 2, 3), (7, 6, 5, 4)
REST = SECOND + THIRD
EVEN, ODD = (0,), (1,)
BOTH = (0, 1)


def kernel(
    n_tile,
    n_lev,
    traj_hbm,
    inc_hbm,
    counts_hbm,
    kappa_hbm,
    courant_hbm,
    vertical_hbm,
    offset_hbm,
    weight_hbm,
    tangent_out,
    grad_out,
    traj_ref,
    inc_ref,
    counts_ref,
    kappa_ref,
    courant_ref,
    vertical_ref,
    offset_ref,
    weight,
    shifted,
    fields,
    outgoing,
    mixing,
    summed,
    recv,
    coef,
    delta,
    loss,
    tang,
    up_out,
    down_out,
    below_in,
    above_in,
    tiny_out,
    tiny_in,
    turn,
    adj,
    back,
    placed,
    load_sem,
    weight_sem,
    fwd_send,
    fwd_recv,
    coef_send,
    coef_recv,
    tiny_send,
    tiny_recv,
    lev_send,
    lev_recv,
    ret_recv,
):
    tracers, levels, cols = traj_hbm.shape
    rows = tracers * levels
    reach = weight_hbm.shape[1]
    win, cap = weight_hbm.shape[2], weight_hbm.shape[3]
    centre = reach // 2
    span = cols // reach
    tiles = cols // LANES
    sub = span // LANES
    me = lax.axis_index("tile")
    lev = lax.axis_index("lev")

    def tile_at(distance):
        return (lax.rem(me + (n_tile + distance), n_tile), lev)

    barrier = pltpu.get_barrier_semaphore()
    radius = centre + 1
    for distance in range(-radius, radius + 1):
        if distance != 0:
            pl.semaphore_signal(barrier, inc=1, device_id=tile_at(distance), device_id_type=MESH)

    @pl.when(lev > 0)
    def _():
        pl.semaphore_signal(barrier, inc=1, device_id=(me, lev - 1), device_id_type=MESH)

    @pl.when(lev < n_lev - 1)
    def _():
        pl.semaphore_signal(barrier, inc=1, device_id=(me, lev + 1), device_id_type=MESH)

    loads = [
        pltpu.make_async_copy(source, target, load_sem.at[i])
        for i, (source, target) in enumerate(
            (
                (counts_hbm, counts_ref),
                (kappa_hbm, kappa_ref),
                (traj_hbm, traj_ref),
                (inc_hbm, inc_ref),
                (courant_hbm, courant_ref),
                (vertical_hbm, vertical_ref),
                (offset_hbm, offset_ref),
            )
        )
    ]
    weight_copies = {
        d: pltpu.make_async_copy(weight_hbm.at[0, d], weight.at[d], sem)
        for group, sems in ((FIRST, weight_sem), (REST, load_sem))
        for d, sem in ((d, sems.at[i]) for i, d in enumerate(group))
    }
    for copy in loads:
        copy.start()
    for d in FIRST:
        weight_copies[d].start()

    for copy in loads:
        copy.wait()
    for d in REST:
        weight_copies[d].start()
    stacked = jnp.concatenate(
        [ref[m].astype(jnp.float32) for ref in (traj_ref, inc_ref) for m in range(tracers)], axis=0
    ).astype(jnp.bfloat16)
    for t in range(tiles):
        fields[t] = stacked[:, t * LANES : (t + 1) * LANES]
    for t in range(tiles, fields.shape[0]):
        fields[t] = jnp.zeros((2 * rows, LANES), jnp.bfloat16)
    vertical = vertical_ref[...]
    coef[pl.ds(0, 1), pl.ds(LANES, cols)] = courant_ref[...]
    coef[pl.ds(1, 1), pl.ds(LANES, cols)] = offset_ref[...].astype(jnp.float32)
    coef[pl.ds(2, 1), pl.ds(LANES, cols)] = jnp.maximum(vertical, 0.0)
    coef[pl.ds(3, 1), pl.ds(LANES, cols)] = jnp.maximum(-vertical, 0.0)
    coef[pl.ds(4, 4), pl.ds(LANES, cols)] = jnp.zeros((4, cols), jnp.float32)
    for ref in (up_out, down_out):
        ref[pl.ds(6, 2), :] = jnp.zeros((2, ref.shape[1]), jnp.float32)
    turn[...] = jnp.zeros_like(turn)
    for at in (0, delta.shape[1] - LANES):
        delta[:, pl.ds(at, LANES)] = jnp.zeros((rows, LANES), jnp.float32)

    @pl.when(lev == 0)
    def _():
        below_in[...] = jnp.zeros_like(below_in)

    @pl.when(lev == n_lev - 1)
    def _():
        above_in[...] = jnp.zeros_like(above_in)

    placed[:, pl.ds(0, 1)] = jnp.zeros((reach, 1, rows, LANES), jnp.float32)
    placed[:, pl.ds(placed.shape[1] - 1, 1)] = jnp.zeros((reach, 1, rows, LANES), jnp.float32)

    starts = []
    total = jnp.int32(0)
    for d in range(reach):
        starts.append(total)
        total = total + counts_ref[0, d]

    firsts = [lax.shift_right_logical(start, 7) for start in starts]
    shifts = [lax.bitwise_and(start, LANES - 1) for start in starts]
    parts = cap // LANES
    lane = lax.broadcasted_iota(jnp.int32, (2 * rows, LANES), 1)
    skew = lax.broadcasted_iota(jnp.int32, (2 * LANES, LANES), 0) - lax.broadcasted_iota(
        jnp.int32, (2 * LANES, LANES), 1
    )

    def selection(amount):
        return jnp.where(skew == amount, 1.0, 0.0).astype(jnp.bfloat16)

    def slots_of(d):
        loaded = [fields[firsts[d] + t] for t in range(parts + 1)]
        pairs = [jnp.concatenate([loaded[t], loaded[t + 1]], axis=1) for t in range(parts)]
        moved = jnp.dot(
            jnp.concatenate(pairs, axis=0), selection(shifts[d]), preferred_element_type=jnp.float32
        )
        pieces = []
        for t in range(parts):
            value = moved[t * 2 * rows : (t + 1) * 2 * rows]
            pieces.append(jnp.where(lane + t * LANES < counts_ref[0, d], value, 0.0).astype(jnp.bfloat16))
        return jnp.concatenate(pieces, axis=1)

    tall = lax.broadcasted_iota(jnp.int32, (win, LANES), 1)

    def place_weight(d):
        chosen = selection(LANES - shifts[d])
        nothing = jnp.zeros((win, LANES), jnp.bfloat16)
        live = []
        for t in range(parts):
            piece = weight[d, :, pl.ds(t * LANES, LANES)]
            live.append(jnp.where(tall + t * LANES < counts_ref[0, d], piece, nothing))
        live = [nothing, *live, nothing]
        for t in range(parts + 1):
            moved = jnp.dot(
                jnp.concatenate([live[t], live[t + 1]], axis=1), chosen, preferred_element_type=jnp.float32
            )
            shifted[d, :, pl.ds(t * LANES, LANES)] = moved.astype(jnp.bfloat16)

    parity = lax.rem(me, 2)
    half = win // 2

    def on_core(cores, run):
        if len(cores) == 2:
            run()
        else:
            pl.when(parity == cores[0])(run)

    def window_part(d, lane, width):
        part = pl.ds(lane, width)
        return outgoing.at[d, :, part], recv.at[d, :, part], d - centre

    plan = {
        "g0l": (BOTH, 0, 0, *window_part(0, 0, half)),
        "g2h": (EVEN, 2, 2, *window_part(2, half, half)),
        "g3h": (EVEN, 3, 3, *window_part(3, half, half)),
        "g3w": (ODD, 3, 3, *window_part(3, 0, win)),
        "g5w": (EVEN, 4, 4, *window_part(5, 0, win)),
        "g5l": (ODD, 4, 4, *window_part(5, 0, half)),
        "g6h": (EVEN, 5, 5, *window_part(6, half, half)),
        "g6l": (ODD, 5, 5, *window_part(6, 0, half)),
        "g7h": (EVEN, 6, 6, *window_part(7, half, half)),
        "g7w": (ODD, 6, 6, *window_part(7, 0, win)),
        "m1": (EVEN, 7, 10, outgoing.at[1, :, pl.ds(0, half)], mixing.at[0], 1),
        "m2": (EVEN, 8, 11, outgoing.at[2, :, pl.ds(0, half)], mixing.at[1], 1),
        "m3": (EVEN, 9, 12, outgoing.at[3, :, pl.ds(0, half)], mixing.at[2], 1),
        "m5": (ODD, 7, 10, outgoing.at[5, :, pl.ds(half, half)], mixing.at[0], -1),
        "m6": (ODD, 8, 11, outgoing.at[6, :, pl.ds(half, half)], mixing.at[1], -1),
        "t0": (EVEN, 1, 1, outgoing.at[0, :, pl.ds(half, half)], mixing.at[3], -1),
        "t1": (EVEN, 12, 13, outgoing.at[1, :, pl.ds(half, half)], mixing.at[4], -1),
        "u1": (ODD, 1, 1, summed.at[3], recv.at[1, :, pl.ds(0, half)], -3),
        "u2": (ODD, 2, 2, summed.at[4], recv.at[2, :, pl.ds(0, half)], -2),
        "c1": (ODD, 9, 7, summed.at[0], recv.at[1, :, pl.ds(0, half)], -4),
        "c2": (ODD, 10, 7, summed.at[1], recv.at[2, :, pl.ds(0, half)], -3),
        "c3": (ODD, 11, 8, summed.at[2], recv.at[3, :, pl.ds(0, half)], -2),
        "c6": (EVEN, 10, 8, summed.at[0], recv.at[6, :, pl.ds(0, half)], 2),
        "c7": (EVEN, 11, 9, summed.at[1], recv.at[7, :, pl.ds(0, half)], 3),
    }
    forward = {
        name: pltpu.make_async_remote_copy(
            src_ref=source,
            dst_ref=target,
            send_sem=fwd_send.at[leaving],
            recv_sem=fwd_recv.at[landing],
            device_id=tile_at(distance),
            device_id_type=MESH,
        )
        for name, (_, leaving, landing, source, target, distance) in plan.items()
    }
    corners = ((0, 0, 0, -5), (7, half, 0, 2), (7, half - 16, 8, 4), (6, win - 16, 8, 3))
    halo_parts = [
        pltpu.make_async_remote_copy(
            src_ref=tiny_out.at[i],
            dst_ref=tiny_in.at[i],
            send_sem=tiny_send.at[i],
            recv_sem=tiny_recv.at[i],
            device_id=tile_at(distance),
            device_id_type=MESH,
        )
        for i, (_, _, _, distance) in enumerate(corners)
    ]

    def send(*names):
        for name in names:
            on_core(plan[name][0], forward[name].start)

    def arrived(*names):
        for name in names:
            forward[name].wait_recv()

    giving = {
        d: pltpu.make_async_remote_copy(
            src_ref=adj.at[:, pl.ds(d * span, win)],
            dst_ref=back.at[d],
            send_sem=fwd_send.at[d if d < centre else d - 1],
            recv_sem=ret_recv.at[d],
            device_id=tile_at(centre - d),
            device_id_type=MESH,
        )
        for d in range(reach)
        if d != centre
    }

    coef_edges = [
        pltpu.make_async_remote_copy(
            src_ref=coef.at[:, pl.ds(source, LANES)],
            dst_ref=coef.at[:, pl.ds(target, LANES)],
            send_sem=coef_send.at[i],
            recv_sem=coef_recv.at[i],
            device_id=tile_at(distance),
            device_id_type=MESH,
        )
        for i, (source, target, distance) in enumerate(((LANES, LANES + cols, -1), (cols, 0, 1)))
    ]

    early = ((-1, 1), (11, tiles + 1))
    middle = ((1, 5),)
    late = ((5, 11),)
    level_up, level_down = ([], [], []), ([], [], [])
    index = 0
    for stage, ranges in enumerate((early, middle, late)):
        for lo, hi in ranges:
            part = pl.ds((lo + 1) * LANES, (hi - lo) * LANES)
            for ways, source, target, distance in (
                (level_up, up_out, below_in, 1),
                (level_down, down_out, above_in, n_lev - 1),
            ):
                ways[stage].append(
                    pltpu.make_async_remote_copy(
                        src_ref=source.at[:, part],
                        dst_ref=target.at[:, part],
                        send_sem=lev_send.at[index],
                        recv_sem=lev_recv.at[index],
                        device_id=(me, lax.rem(lev + distance, n_lev)),
                        device_id_type=MESH,
                    )
                )
                index += 1

    def level_start(stage):
        @pl.when(lev < n_lev - 1)
        def _():
            for copy in level_up[stage]:
                copy.start()

        @pl.when(lev > 0)
        def _():
            for copy in level_down[stage]:
                copy.start()

    def level_wait(stage):
        @pl.when(lev > 0)
        def _():
            for copy in level_up[stage]:
                copy.wait_recv()

        @pl.when(lev < n_lev - 1)
        def _():
            for copy in level_down[stage]:
                copy.wait_recv()

    sends = {
        0: ("g0l", "t0"),
        7: ("g7h", "g7w"),
        6: ("m6", "g6h", "g6l"),
        1: ("m1", "t1"),
        2: ("m2", "g2h"),
        3: ("m3", "g3h", "g3w"),
        5: ("m5", "g5w", "g5l"),
    }

    def windows(groups):
        slotted = {d: slots_of(d) for d in groups}
        for d in groups:
            weight_copies[d].wait()
        for i, (d, column, row, _) in enumerate(corners):
            if d in groups:
                corner = lax.dot_general(
                    weight[d, pl.ds(column, 16), :],
                    slotted[d],
                    (((1,), (1,)), ((), ())),
                    preferred_element_type=jnp.float32,
                )
                tiny_out[i, :, pl.ds(0, 2 * rows)] = corner[row : row + 8]
        for d in groups:
            window = lax.dot_general(
                slotted[d], weight[d], (((1,), (1,)), ((), ())), preferred_element_type=jnp.float32
            )
            if d == centre:
                recv[d] = window
            else:
                outgoing[d] = window

    tiny_out[...] = jnp.zeros_like(tiny_out)
    windows(FIRST)
    pl.semaphore_wait(
        barrier, 2 * radius + (lev > 0).astype(jnp.int32) + (lev < n_lev - 1).astype(jnp.int32)
    )
    for copy in coef_edges:
        copy.start()

    def send_group(group):
        for copy, corner in zip(halo_parts, corners):
            if corner[0] in group:
                copy.start()
        for d in group:
            if d != centre:
                send(*sends[d])

    send_group(FIRST)
    for group in (SECOND, THIRD):
        windows(group)
        send_group(group)
    for d in SECOND:
        place_weight(d)

    @pl.when(parity == 1)
    def _():
        for name, slot, d, at, sum_name in (
            ("m1", 0, 0, half, "c1"),
            ("t0", 3, 1, 0, "u1"),
            ("m2", 1, 1, half, "c2"),
            ("t1", 4, 2, 0, "u2"),
            ("m3", 2, 2, half, "c3"),
        ):
            forward[name].wait_recv()
            summed[slot] = outgoing[d, :, pl.ds(at, half)] + mixing[slot]
            forward[sum_name].start()

    @pl.when(parity == 0)
    def _():
        arrived("m6")
        summed[1] = outgoing[7, :, pl.ds(0, half)] + mixing[1]
        forward["c7"].start()
        arrived("m5")
        summed[0] = outgoing[6, :, pl.ds(0, half)] + mixing[0]
        forward["c6"].start()

    def finish(column, width, *pieces):
        value = None
        for d, at in pieces:
            piece = recv[d, :, pl.ds(at, width)]
            value = piece if value is None else value + piece
        for m in range(tracers):
            part = pl.ds(m * levels, levels)
            loss[part, pl.ds(LANES + column, width)] = 2.0 * kappa_ref[m] * value[m * levels : (m + 1) * levels]
        delta[:, pl.ds(2 * LANES + column, width)] = value[rows:]

    def finish_halo():
        turn[pl.ds(0, 8), :] = tiny_in[0] + tiny_in[1]
        turn[pl.ds(LANES - 8, 8), :] = tiny_in[2] + tiny_in[3]
        value = jnp.transpose(turn[...])
        for at in (0, LANES + cols):
            for m in range(tracers):
                part = pl.ds(m * levels, levels)
                loss[part, pl.ds(at, LANES)] = 2.0 * kappa_ref[m] * value[m * levels : (m + 1) * levels]
            delta[:, pl.ds(LANES + at, LANES)] = value[rows : 2 * rows]

    def level_rows(width):
        return lax.broadcasted_iota(jnp.int32, (levels, width), 0)

    def tangent_partial(lo, hi):
        width = (hi - lo) * LANES
        own = pl.ds(LANES + lo * LANES, width)
        courant, offset = coef[pl.ds(0, 1), own], coef[pl.ds(1, 1), own]
        rising, sinking = coef[pl.ds(2, 1), own], coef[pl.ds(3, 1), own]
        level = level_rows(width)
        for m in range(tracers):
            part = pl.ds(m * levels, levels)
            wide = delta[part, pl.ds((lo + 1) * LANES, width + 2 * LANES)]
            here = wide[:, LANES : LANES + width]
            departed = jnp.zeros_like(here)
            for shift in range(-HALO, HALO + 1):
                moved = here
                if shift != 0:
                    moved = pltpu.roll(wide, (-shift) % (width + 2 * LANES), 1)[:, LANES : LANES + width]
                departed = jnp.where(offset == float(shift), moved, departed)
            below = jnp.where(level == 0, 0.0, pltpu.roll(here, 1, 0))
            above = jnp.where(level == levels - 1, 0.0, pltpu.roll(here, levels - 1, 0))
            value = (
                here
                + courant * (departed - here)
                + rising * (below - here)
                + sinking * (above - here)
                - loss[part, own] * here
            )
            tang[part, own] = value
            up_out[pl.ds(m, 1), own] = value[levels - 1 : levels]
            up_out[pl.ds(tracers + m, 1), own] = here[levels - 1 : levels]
            down_out[pl.ds(m, 1), own] = value[0:1]
            down_out[pl.ds(tracers + m, 1), own] = here[0:1]

    def tangent_finish(lo, hi):
        width = (hi - lo) * LANES
        own = pl.ds(LANES + lo * LANES, width)
        rising, sinking = coef[pl.ds(2, 1), own], coef[pl.ds(3, 1), own]
        level = level_rows(width)
        inner_lo, inner_hi = max(lo, 0), min(hi, tiles)
        for m in range(tracers):
            part = pl.ds(m * levels, levels)
            value = tang[part, own]
            value = value + jnp.where(level == 0, rising * below_in[pl.ds(tracers + m, 1), own], 0.0)
            value = value + jnp.where(level == levels - 1, sinking * above_in[pl.ds(tracers + m, 1), own], 0.0)
            tang[part, own] = value
            tangent_out[m, :, pl.ds(inner_lo * LANES, (inner_hi - inner_lo) * LANES)] = value[
                :, (inner_lo - lo) * LANES : (inner_hi - lo) * LANES
            ]

    def adjoint(lo, hi):
        width = (hi - lo) * LANES
        own = pl.ds(LANES + lo * LANES, width)
        out = pl.ds(lo * LANES, width)
        around = pl.ds(lo * LANES, width + 2 * LANES)
        courant, rising, sinking = coef[pl.ds(0, 1), own], coef[pl.ds(2, 1), own], coef[pl.ds(3, 1), own]
        wide_courant, wide_offset = coef[pl.ds(0, 1), around], coef[pl.ds(1, 1), around]
        level = level_rows(width)
        pieces = []
        for m in range(tracers):
            part = pl.ds(m * levels, levels)
            wide = tang[part, around]
            here = wide[:, LANES : LANES + width]
            total = jnp.zeros_like(here)
            for shift in range(-HALO, HALO + 1):
                term = jnp.where(wide_offset == float(shift), wide_courant, 0.0) * wide
                if shift != 0:
                    term = pltpu.roll(term, shift % (width + 2 * LANES), 1)
                total = total + term[:, LANES : LANES + width]
            own_delta = delta[part, pl.ds((lo + 2) * LANES, width)]
            under = below_in[pl.ds(m, 1), own] + sinking * own_delta[0:1]
            over = above_in[pl.ds(m, 1), own] + rising * own_delta[levels - 1 : levels]
            under = jnp.where(lev > 0, under, 0.0)
            over = jnp.where(lev < n_lev - 1, over, 0.0)
            lower = jnp.where(level == 0, under, pltpu.roll(here, 1, 0))
            upper = jnp.where(level == levels - 1, over, pltpu.roll(here, levels - 1, 0))
            diagonal = 1.0 - courant - rising - sinking - loss[part, own]
            pieces.append(diagonal * here + total + rising * upper + sinking * lower)
        value = jnp.concatenate(pieces, axis=0).astype(jnp.bfloat16)
        adj[:, out] = value
        if lo == 0:
            adj[:, pl.ds(cols, span)] = value[:, :span]

    for d in FIRST + THIRD:
        place_weight(d)
    for copy in (*halo_parts, *coef_edges):
        copy.wait_recv()
    finish_halo()

    @pl.when(parity == 0)
    def _():
        arrived("g0l", "g7w", "g6h", "g5l", "c6")
        finish(0, span, (0, 0), (7, half))
        finish(7 * span, span, (7, 0), (6, half))
        finish(5 * span, span, (5, 0), (4, half))
        finish(6 * span, span, (6, 0))

    @pl.when(parity == 1)
    def _():
        arrived("g0l", "g7h", "c7", "g6l", "g5w")
        finish(0, span, (0, 0), (7, half))
        finish(7 * span, span, (7, 0))
        finish(5 * span, span, (5, 0), (4, half))
        finish(6 * span, span, (6, 0), (5, half))

    for lo, hi in early:
        tangent_partial(lo, hi)
    level_start(0)

    @pl.when(parity == 0)
    def _():
        arrived("u1", "c2")
        finish(span, span, (1, 0))
        finish(2 * span, span, (2, 0))

    @pl.when(parity == 1)
    def _():
        arrived("c1", "u2")
        finish(span, span, (1, 0))
        finish(2 * span, span, (2, 0))

    for lo, hi in middle:
        tangent_partial(lo, hi)
    level_start(1)

    @pl.when(parity == 0)
    def _():
        arrived("g2h", "g3w")
        finish(3 * span, span, (3, 0), (2, half))
        finish(4 * span, span, (4, 0), (3, half))

    @pl.when(parity == 1)
    def _():
        arrived("g3h", "c3")
        finish(3 * span, span, (3, 0))
        finish(4 * span, span, (4, 0), (3, half))

    for lo, hi in late:
        tangent_partial(lo, hi)
    level_start(2)
    level_wait(0)
    for lo, hi in early:
        tangent_finish(lo, hi)
    level_wait(1)
    for lo, hi in middle:
        tangent_finish(lo, hi)
    adjoint(0, 4)
    adjoint(12, tiles)
    for name, copy in forward.items():
        on_core(plan[name][0], copy.wait_send)
    for d in (0, 7, 6):
        giving[d].start()
    level_wait(2)
    for lo, hi in late:
        tangent_finish(lo, hi)
    adjoint(4, 12)
    for d in (1, 2, 5, 3):
        giving[d].start()

    def grads(groups):
        for d in groups:
            if d != centre:
                giving[d].wait_recv()
        for d in groups:
            returned = adj[:, pl.ds(d * span, win)] if d == centre else back[d]
            grad = jnp.dot(returned, shifted[d], preferred_element_type=jnp.float32)
            for t in range(parts + 1):
                placed[d, t + 1] = grad[:, t * LANES : (t + 1) * LANES]

    top = placed.shape[1] - 1

    def unslot(groups, again):
        for t in range(tiles):
            value = None
            for d in groups:
                piece = placed[d, lax.min(lax.max(t + 1 - firsts[d], 0), top)]
                value = piece if value is None else value + piece
            for m in range(tracers):
                part = value[m * levels : (m + 1) * levels]
                if again:
                    part = part + grad_out[m, :, pl.ds(t * LANES, LANES)]
                grad_out[m, :, pl.ds(t * LANES, LANES)] = part

    for again, groups in ((False, (centre, 0, 7, 6)), (True, (1, 2, 5, 3))):
        grads(groups)
        unslot(groups, again)

    for copy in (*giving.values(), *coef_edges, *halo_parts):
        copy.wait_send()

    @pl.when(lev < n_lev - 1)
    def _():
        for copies in level_up:
            for copy in copies:
                copy.wait_send()

    @pl.when(lev > 0)
    def _():
        for copies in level_down:
            for copy in copies:
                copy.wait_send()


def store(tangent_ref, grad_ref, tangent_hbm, grad_hbm, sem):
    copies = [
        pltpu.make_async_copy(tangent_ref, tangent_hbm, sem.at[0]),
        pltpu.make_async_copy(grad_ref, grad_hbm, sem.at[1]),
    ]
    for copy in copies:
        copy.start()
    for copy in copies:
        copy.wait()


def shards(n_tile, n_lev, trajectory, increment, counts, remap_weight, kappa, courant, vertical, offset):
    tracers, levels, cols = trajectory.shape
    reach, win, cap = remap_weight.shape[1:]
    rows = tracers * levels
    span = cols // reach
    wide = cols + 2 * LANES
    f32, bf16 = jnp.float32, jnp.bfloat16
    vmem = pl.BlockSpec(memory_space=pltpu.VMEM)
    dma = pltpu.SemaphoreType.DMA
    out = jax.ShapeDtypeStruct((tracers, levels, cols), f32)
    results = pl.pallas_call(
        functools.partial(kernel, n_tile, n_lev),
        out_shape=(out, out),
        in_specs=[pl.BlockSpec(memory_space=pltpu.HBM)] * 8,
        out_specs=(vmem, vmem),
        scratch_shapes=[
            pltpu.VMEM((tracers, levels, cols), bf16),
            pltpu.VMEM((tracers, levels, cols), bf16),
            pltpu.SMEM((1, reach), jnp.int32),
            pltpu.SMEM((tracers,), f32),
            pltpu.VMEM((1, cols), f32),
            pltpu.VMEM((1, cols), f32),
            pltpu.VMEM((1, cols), jnp.int32),
            pltpu.VMEM((reach, win, cap), bf16),
            pltpu.VMEM((reach, win, cap + LANES), bf16),
            pltpu.VMEM((cols // LANES + cap // LANES + 1, 2 * rows, LANES), bf16),
            pltpu.VMEM((reach, 2 * rows, win), f32),
            pltpu.VMEM((5, 2 * rows, win // 2), f32),
            pltpu.VMEM((5, 2 * rows, win // 2), f32),
            pltpu.VMEM((reach, 2 * rows, win), f32),
            pltpu.VMEM((8, wide), f32),
            pltpu.VMEM((rows, wide + 2 * LANES), f32),
            pltpu.VMEM((rows, wide), f32),
            pltpu.VMEM((rows, wide), f32),
            pltpu.VMEM((8, wide), f32),
            pltpu.VMEM((8, wide), f32),
            pltpu.VMEM((8, wide), f32),
            pltpu.VMEM((8, wide), f32),
            pltpu.VMEM((4, 8, LANES), f32),
            pltpu.VMEM((4, 8, LANES), f32),
            pltpu.VMEM((LANES, LANES), f32),
            pltpu.VMEM((rows, cols + span), bf16),
            pltpu.VMEM((reach, rows, win), bf16),
            pltpu.VMEM((reach, cap // LANES + 3, rows, LANES), f32),
            dma((7,)),
            dma((len(FIRST),)),
            dma((13,)),
            dma((14,)),
            dma((2,)),
            dma((2,)),
            dma((4,)),
            dma((4,)),
            dma((8,)),
            dma((8,)),
            dma((reach,)),
        ],
        compiler_params=pltpu.CompilerParams(
            collective_id=0, has_side_effects=True, vmem_limit_bytes=24 * 1024 * 1024
        ),
    )(
        *(
            pltpu.with_memory_space_constraint(operand, pltpu.HBM)
            for operand in (
                trajectory,
                increment,
                counts,
                kappa,
                courant.reshape(1, cols),
                vertical.reshape(1, cols),
                offset.reshape(1, cols),
                remap_weight,
            )
        )
    )
    return pl.pallas_call(
        store,
        out_shape=(out, out),
        in_specs=(vmem, vmem),
        out_specs=[pl.BlockSpec(memory_space=pltpu.HBM)] * 2,
        scratch_shapes=[dma((2,))],
        compiler_params=pltpu.CompilerParams(vmem_limit_bytes=1024 * 1024),
    )(*results)


def solution(mesh):
    return jax.shard_map(
        functools.partial(shards, mesh.shape["tile"], mesh.shape["lev"]),
        mesh=mesh,
        in_specs=(
            P(None, "lev", "tile"),
            P(None, "lev", "tile"),
            P("tile", None),
            P("tile", None, None, None),
            P(),
            P("tile"),
            P("tile"),
            P("tile"),
        ),
        out_specs=(P(None, "lev", "tile"), P(None, "lev", "tile")),
        check_vma=False,
    )
```

```python
import functools

import jax
import jax.numpy as jnp
from jax import lax
from jax.experimental import pallas as pl
from jax.experimental.pallas import tpu as pltpu
from jax.sharding import PartitionSpec as P

MESH = pl.DeviceIdType.MESH
LANES = 128
HALO = 2
FIRST, SECOND, THIRD = (0,), (7, 6, 1), (2, 3, 5, 4)
REST = SECOND + THIRD
EVEN, ODD = (0,), (1,)
BOTH = (0, 1)


def kernel(
    n_tile,
    n_lev,
    traj_hbm,
    inc_hbm,
    counts_hbm,
    kappa_hbm,
    courant_hbm,
    vertical_hbm,
    offset_hbm,
    weight_hbm,
    tangent_out,
    grad_out,
    traj_ref,
    inc_ref,
    counts_ref,
    kappa_ref,
    courant_ref,
    vertical_ref,
    offset_ref,
    weight,
    shifted,
    fields,
    outgoing,
    mixing,
    summed,
    recv,
    coef,
    delta,
    loss,
    tang,
    up_out,
    down_out,
    below_in,
    above_in,
    tiny_out,
    tiny_in,
    turn,
    adj,
    back,
    placed,
    load_sem,
    weight_sem,
    fwd_send,
    fwd_recv,
    coef_send,
    coef_recv,
    tiny_send,
    tiny_recv,
    lev_send,
    lev_recv,
    ret_recv,
):
    tracers, levels, cols = traj_hbm.shape
    rows = tracers * levels
    reach = weight_hbm.shape[1]
    win, cap = weight_hbm.shape[2], weight_hbm.shape[3]
    centre = reach // 2
    span = cols // reach
    tiles = cols // LANES
    sub = span // LANES
    me = lax.axis_index("tile")
    lev = lax.axis_index("lev")

    def tile_at(distance):
        return (lax.rem(me + (n_tile + distance), n_tile), lev)

    barrier = pltpu.get_barrier_semaphore()
    radius = centre + 1
    for distance in range(-radius, radius + 1):
        if distance != 0:
            pl.semaphore_signal(barrier, inc=1, device_id=tile_at(distance), device_id_type=MESH)

    @pl.when(lev > 0)
    def _():
        pl.semaphore_signal(barrier, inc=1, device_id=(me, lev - 1), device_id_type=MESH)

    @pl.when(lev < n_lev - 1)
    def _():
        pl.semaphore_signal(barrier, inc=1, device_id=(me, lev + 1), device_id_type=MESH)

    loads = [
        pltpu.make_async_copy(source, target, load_sem.at[i])
        for i, (source, target) in enumerate(
            (
                (counts_hbm, counts_ref),
                (kappa_hbm, kappa_ref),
                (traj_hbm, traj_ref),
                (inc_hbm, inc_ref),
                (courant_hbm, courant_ref),
                (vertical_hbm, vertical_ref),
                (offset_hbm, offset_ref),
            )
        )
    ]
    weight_copies = {
        d: pltpu.make_async_copy(weight_hbm.at[0, d], weight.at[d], sem)
        for group, sems in ((FIRST, weight_sem), (REST, load_sem))
        for d, sem in ((d, sems.at[i]) for i, d in enumerate(group))
    }
    for copy in loads:
        copy.start()
    for d in FIRST:
        weight_copies[d].start()

    for copy in loads:
        copy.wait()
    for d in REST:
        weight_copies[d].start()
    stacked = jnp.concatenate(
        [ref[m].astype(jnp.float32) for ref in (traj_ref, inc_ref) for m in range(tracers)], axis=0
    ).astype(jnp.bfloat16)
    for t in range(tiles):
        fields[t] = stacked[:, t * LANES : (t + 1) * LANES]
    for t in range(tiles, fields.shape[0]):
        fields[t] = jnp.zeros((2 * rows, LANES), jnp.bfloat16)
    vertical = vertical_ref[...]
    coef[pl.ds(0, 1), pl.ds(LANES, cols)] = courant_ref[...]
    coef[pl.ds(1, 1), pl.ds(LANES, cols)] = offset_ref[...].astype(jnp.float32)
    coef[pl.ds(2, 1), pl.ds(LANES, cols)] = jnp.maximum(vertical, 0.0)
    coef[pl.ds(3, 1), pl.ds(LANES, cols)] = jnp.maximum(-vertical, 0.0)
    coef[pl.ds(4, 4), pl.ds(LANES, cols)] = jnp.zeros((4, cols), jnp.float32)
    for ref in (up_out, down_out):
        ref[pl.ds(6, 2), :] = jnp.zeros((2, ref.shape[1]), jnp.float32)
    turn[...] = jnp.zeros_like(turn)
    for at in (0, delta.shape[1] - LANES):
        delta[:, pl.ds(at, LANES)] = jnp.zeros((rows, LANES), jnp.float32)

    @pl.when(lev == 0)
    def _():
        below_in[...] = jnp.zeros_like(below_in)

    @pl.when(lev == n_lev - 1)
    def _():
        above_in[...] = jnp.zeros_like(above_in)

    placed[:, pl.ds(0, 1)] = jnp.zeros((reach, 1, rows, LANES), jnp.float32)
    placed[:, pl.ds(placed.shape[1] - 1, 1)] = jnp.zeros((reach, 1, rows, LANES), jnp.float32)

    starts = []
    total = jnp.int32(0)
    for d in range(reach):
        starts.append(total)
        total = total + counts_ref[0, d]

    firsts = [lax.shift_right_logical(start, 7) for start in starts]
    shifts = [lax.bitwise_and(start, LANES - 1) for start in starts]
    parts = cap // LANES
    lane = lax.broadcasted_iota(jnp.int32, (2 * rows, LANES), 1)
    skew = lax.broadcasted_iota(jnp.int32, (2 * LANES, LANES), 0) - lax.broadcasted_iota(
        jnp.int32, (2 * LANES, LANES), 1
    )

    def selection(amount):
        return jnp.where(skew == amount, 1.0, 0.0).astype(jnp.bfloat16)

    def slots_of(d):
        loaded = [fields[firsts[d] + t] for t in range(parts + 1)]
        pairs = [jnp.concatenate([loaded[t], loaded[t + 1]], axis=1) for t in range(parts)]
        moved = jnp.dot(
            jnp.concatenate(pairs, axis=0), selection(shifts[d]), preferred_element_type=jnp.float32
        )
        pieces = []
        for t in range(parts):
            value = moved[t * 2 * rows : (t + 1) * 2 * rows]
            pieces.append(jnp.where(lane + t * LANES < counts_ref[0, d], value, 0.0).astype(jnp.bfloat16))
        return jnp.concatenate(pieces, axis=1)

    tall = lax.broadcasted_iota(jnp.int32, (win, LANES), 1)

    def place_weight(d):
        chosen = selection(LANES - shifts[d])
        nothing = jnp.zeros((win, LANES), jnp.bfloat16)
        live = []
        for t in range(parts):
            piece = weight[d, :, pl.ds(t * LANES, LANES)]
            live.append(jnp.where(tall + t * LANES < counts_ref[0, d], piece, nothing))
        live = [nothing, *live, nothing]
        for t in range(parts + 1):
            moved = jnp.dot(
                jnp.concatenate([live[t], live[t + 1]], axis=1), chosen, preferred_element_type=jnp.float32
            )
            shifted[d, :, pl.ds(t * LANES, LANES)] = moved.astype(jnp.bfloat16)

    parity = lax.rem(me, 2)
    half = win // 2

    def on_core(cores, run):
        if len(cores) == 2:
            run()
        else:
            pl.when(parity == cores[0])(run)

    def window_part(d, lane, width):
        part = pl.ds(lane, width)
        return outgoing.at[d, :, part], recv.at[d, :, part], d - centre

    plan = {
        "g0l": (BOTH, 0, 0, *window_part(0, 0, half)),
        "g2h": (EVEN, 2, 2, *window_part(2, half, half)),
        "g3h": (EVEN, 3, 3, *window_part(3, half, half)),
        "g3w": (ODD, 3, 3, *window_part(3, 0, win)),
        "g5w": (EVEN, 4, 4, *window_part(5, 0, win)),
        "g5l": (ODD, 4, 4, *window_part(5, 0, half)),
        "g6l": (ODD, 5, 5, *window_part(6, 0, half)),
        "g7h": (BOTH, 6, 6, *window_part(7, half, half)),
        "m1": (EVEN, 7, 10, outgoing.at[1, :, pl.ds(0, half)], mixing.at[0], 1),
        "m2": (EVEN, 8, 11, outgoing.at[2, :, pl.ds(0, half)], mixing.at[1], 1),
        "m3": (EVEN, 9, 12, outgoing.at[3, :, pl.ds(0, half)], mixing.at[2], 1),
        "m5": (ODD, 7, 10, outgoing.at[5, :, pl.ds(half, half)], mixing.at[0], -1),
        "m6": (ODD, 8, 11, outgoing.at[6, :, pl.ds(half, half)], mixing.at[1], -1),
        "v7": (ODD, 12, 12, outgoing.at[7, :, pl.ds(0, half)], mixing.at[5], 1),
        "t0": (EVEN, 1, 1, outgoing.at[0, :, pl.ds(half, half)], mixing.at[3], -1),
        "t1": (EVEN, 12, 13, outgoing.at[1, :, pl.ds(half, half)], mixing.at[4], -1),
        "u1": (ODD, 1, 1, summed.at[3], recv.at[1, :, pl.ds(0, half)], -3),
        "u2": (ODD, 2, 2, summed.at[4], recv.at[2, :, pl.ds(0, half)], -2),
        "c1": (ODD, 9, 7, summed.at[0], recv.at[1, :, pl.ds(0, half)], -4),
        "c2": (ODD, 10, 7, summed.at[1], recv.at[2, :, pl.ds(0, half)], -3),
        "c3": (ODD, 11, 8, summed.at[2], recv.at[3, :, pl.ds(0, half)], -2),
        "w7": (EVEN, 5, 5, summed.at[2], recv.at[7, :, pl.ds(0, half)], 2),
        "c6": (EVEN, 10, 8, summed.at[0], recv.at[6, :, pl.ds(0, half)], 2),
        "c7": (EVEN, 11, 9, summed.at[1], recv.at[7, :, pl.ds(0, half)], 3),
    }
    forward = {
        name: pltpu.make_async_remote_copy(
            src_ref=source,
            dst_ref=target,
            send_sem=fwd_send.at[leaving],
            recv_sem=fwd_recv.at[landing],
            device_id=tile_at(distance),
            device_id_type=MESH,
        )
        for name, (_, leaving, landing, source, target, distance) in plan.items()
    }
    corners = ((0, 0, 0, -5), (7, half, 0, 2), (7, half - 16, 8, 4), (6, win - 16, 8, 3))
    halo_parts = [
        pltpu.make_async_remote_copy(
            src_ref=tiny_out.at[i],
            dst_ref=tiny_in.at[i],
            send_sem=tiny_send.at[i],
            recv_sem=tiny_recv.at[i],
            device_id=tile_at(distance),
            device_id_type=MESH,
        )
        for i, (_, _, _, distance) in enumerate(corners)
    ]

    def send(*names):
        for name in names:
            on_core(plan[name][0], forward[name].start)

    def arrived(*names):
        for name in names:
            forward[name].wait_recv()

    giving = {
        d: pltpu.make_async_remote_copy(
            src_ref=adj.at[:, pl.ds(d * span, win)],
            dst_ref=back.at[d],
            send_sem=fwd_send.at[d if d < centre else d - 1],
            recv_sem=ret_recv.at[d],
            device_id=tile_at(centre - d),
            device_id_type=MESH,
        )
        for d in range(reach)
        if d != centre
    }

    coef_edges = [
        pltpu.make_async_remote_copy(
            src_ref=coef.at[:, pl.ds(source, LANES)],
            dst_ref=coef.at[:, pl.ds(target, LANES)],
            send_sem=coef_send.at[i],
            recv_sem=coef_recv.at[i],
            device_id=tile_at(distance),
            device_id_type=MESH,
        )
        for i, (source, target, distance) in enumerate(((LANES, LANES + cols, -1), (cols, 0, 1)))
    ]

    early = ((-1, 1), (11, tiles + 1))
    middle = ((1, 5),)
    late = ((5, 11),)
    level_up, level_down = ([], [], []), ([], [], [])
    index = 0
    for stage, ranges in enumerate((early, middle, late)):
        for lo, hi in ranges:
            part = pl.ds((lo + 1) * LANES, (hi - lo) * LANES)
            for ways, source, target, distance in (
                (level_up, up_out, below_in, 1),
                (level_down, down_out, above_in, n_lev - 1),
            ):
                ways[stage].append(
                    pltpu.make_async_remote_copy(
                        src_ref=source.at[:, part],
                        dst_ref=target.at[:, part],
                        send_sem=lev_send.at[index],
                        recv_sem=lev_recv.at[index],
                        device_id=(me, lax.rem(lev + distance, n_lev)),
                        device_id_type=MESH,
                    )
                )
                index += 1

    def level_start(stage):
        @pl.when(lev < n_lev - 1)
        def _():
            for copy in level_up[stage]:
                copy.start()

        @pl.when(lev > 0)
        def _():
            for copy in level_down[stage]:
                copy.start()

    def level_wait(stage):
        @pl.when(lev > 0)
        def _():
            for copy in level_up[stage]:
                copy.wait_recv()

        @pl.when(lev < n_lev - 1)
        def _():
            for copy in level_down[stage]:
                copy.wait_recv()

    sends = {
        0: ("t0", "g0l"),
        7: ("v7", "g7h"),
        6: ("m6", "g6l"),
        1: ("m1", "t1"),
        2: ("m2", "g2h"),
        3: ("m3", "g3h", "g3w"),
        5: ("m5", "g5w", "g5l"),
    }

    def windows(groups):
        slotted = {d: slots_of(d) for d in groups}
        for d in groups:
            weight_copies[d].wait()
        for i, (d, column, row, _) in enumerate(corners):
            if d in groups:
                corner = lax.dot_general(
                    weight[d, pl.ds(column, 16), :],
                    slotted[d],
                    (((1,), (1,)), ((), ())),
                    preferred_element_type=jnp.float32,
                )
                tiny_out[i, :, pl.ds(0, 2 * rows)] = corner[row : row + 8]
        for d in groups:
            window = lax.dot_general(
                slotted[d], weight[d], (((1,), (1,)), ((), ())), preferred_element_type=jnp.float32
            )
            if d == centre:
                recv[d] = window
            else:
                outgoing[d] = window

    tiny_out[...] = jnp.zeros_like(tiny_out)
    windows(FIRST)
    pl.semaphore_wait(
        barrier, 2 * radius + (lev > 0).astype(jnp.int32) + (lev < n_lev - 1).astype(jnp.int32)
    )
    for copy in coef_edges:
        copy.start()

    def send_group(group):
        for copy, corner in zip(halo_parts, corners):
            if corner[0] in group:
                copy.start()
        for d in group:
            if d != centre:
                send(*sends[d])

    send_group(FIRST)
    for group in (SECOND, THIRD):
        windows(group)
        send_group(group)
    def add(name, slot, d, at, sum_name, mixed):
        forward[name].wait_recv()
        summed[slot] = outgoing[d, :, pl.ds(at, half)] + mixing[mixed]
        forward[sum_name].start()

    for d in (7, 6, 1):
        place_weight(d)

    @pl.when(parity == 1)
    def _():
        add("m1", 0, 0, half, "c1", 0)
        add("m2", 1, 1, half, "c2", 1)
        add("m3", 2, 2, half, "c3", 2)

    @pl.when(parity == 0)
    def _():
        add("m6", 1, 7, 0, "c7", 1)
        add("v7", 2, 6, half, "w7", 5)
        add("m5", 0, 6, 0, "c6", 0)

    for d in (0, 2):
        place_weight(d)

    @pl.when(parity == 1)
    def _():
        add("t0", 3, 1, 0, "u1", 3)

    for d in (3, 5):
        place_weight(d)

    @pl.when(parity == 1)
    def _():
        add("t1", 4, 2, 0, "u2", 4)

    place_weight(centre)

    def finish(column, width, *pieces):
        value = None
        for d, at in pieces:
            piece = recv[d, :, pl.ds(at, width)]
            value = piece if value is None else value + piece
        for m in range(tracers):
            part = pl.ds(m * levels, levels)
            loss[part, pl.ds(LANES + column, width)] = 2.0 * kappa_ref[m] * value[m * levels : (m + 1) * levels]
        delta[:, pl.ds(2 * LANES + column, width)] = value[rows:]

    def finish_halo():
        turn[pl.ds(0, 8), :] = tiny_in[0] + tiny_in[1]
        turn[pl.ds(LANES - 8, 8), :] = tiny_in[2] + tiny_in[3]
        value = jnp.transpose(turn[...])
        for at in (0, LANES + cols):
            for m in range(tracers):
                part = pl.ds(m * levels, levels)
                loss[part, pl.ds(at, LANES)] = 2.0 * kappa_ref[m] * value[m * levels : (m + 1) * levels]
            delta[:, pl.ds(LANES + at, LANES)] = value[rows : 2 * rows]

    def level_rows(width):
        return lax.broadcasted_iota(jnp.int32, (levels, width), 0)

    def tangent_partial(lo, hi):
        width = (hi - lo) * LANES
        own = pl.ds(LANES + lo * LANES, width)
        courant, offset = coef[pl.ds(0, 1), own], coef[pl.ds(1, 1), own]
        rising, sinking = coef[pl.ds(2, 1), own], coef[pl.ds(3, 1), own]
        level = level_rows(width)
        for m in range(tracers):
            part = pl.ds(m * levels, levels)
            wide = delta[part, pl.ds((lo + 1) * LANES, width + 2 * LANES)]
            here = wide[:, LANES : LANES + width]
            departed = jnp.zeros_like(here)
            for shift in range(-HALO, HALO + 1):
                moved = here
                if shift != 0:
                    moved = pltpu.roll(wide, (-shift) % (width + 2 * LANES), 1)[:, LANES : LANES + width]
                departed = jnp.where(offset == float(shift), moved, departed)
            below = jnp.where(level == 0, 0.0, pltpu.roll(here, 1, 0))
            above = jnp.where(level == levels - 1, 0.0, pltpu.roll(here, levels - 1, 0))
            value = (
                here
                + courant * (departed - here)
                + rising * (below - here)
                + sinking * (above - here)
                - loss[part, own] * here
            )
            tang[part, own] = value
            up_out[pl.ds(m, 1), own] = value[levels - 1 : levels]
            up_out[pl.ds(tracers + m, 1), own] = here[levels - 1 : levels]
            down_out[pl.ds(m, 1), own] = value[0:1]
            down_out[pl.ds(tracers + m, 1), own] = here[0:1]

    def tangent_finish(lo, hi):
        width = (hi - lo) * LANES
        own = pl.ds(LANES + lo * LANES, width)
        rising, sinking = coef[pl.ds(2, 1), own], coef[pl.ds(3, 1), own]
        level = level_rows(width)
        inner_lo, inner_hi = max(lo, 0), min(hi, tiles)
        for m in range(tracers):
            part = pl.ds(m * levels, levels)
            value = tang[part, own]
            value = value + jnp.where(level == 0, rising * below_in[pl.ds(tracers + m, 1), own], 0.0)
            value = value + jnp.where(level == levels - 1, sinking * above_in[pl.ds(tracers + m, 1), own], 0.0)
            tang[part, own] = value
            tangent_out[m, :, pl.ds(inner_lo * LANES, (inner_hi - inner_lo) * LANES)] = value[
                :, (inner_lo - lo) * LANES : (inner_hi - lo) * LANES
            ]

    def adjoint(lo, hi):
        width = (hi - lo) * LANES
        own = pl.ds(LANES + lo * LANES, width)
        out = pl.ds(lo * LANES, width)
        around = pl.ds(lo * LANES, width + 2 * LANES)
        courant, rising, sinking = coef[pl.ds(0, 1), own], coef[pl.ds(2, 1), own], coef[pl.ds(3, 1), own]
        wide_courant, wide_offset = coef[pl.ds(0, 1), around], coef[pl.ds(1, 1), around]
        level = level_rows(width)
        pieces = []
        for m in range(tracers):
            part = pl.ds(m * levels, levels)
            wide = tang[part, around]
            here = wide[:, LANES : LANES + width]
            total = jnp.zeros_like(here)
            for shift in range(-HALO, HALO + 1):
                term = jnp.where(wide_offset == float(shift), wide_courant, 0.0) * wide
                if shift != 0:
                    term = pltpu.roll(term, shift % (width + 2 * LANES), 1)
                total = total + term[:, LANES : LANES + width]
            own_delta = delta[part, pl.ds((lo + 2) * LANES, width)]
            under = below_in[pl.ds(m, 1), own] + sinking * own_delta[0:1]
            over = above_in[pl.ds(m, 1), own] + rising * own_delta[levels - 1 : levels]
            under = jnp.where(lev > 0, under, 0.0)
            over = jnp.where(lev < n_lev - 1, over, 0.0)
            lower = jnp.where(level == 0, under, pltpu.roll(here, 1, 0))
            upper = jnp.where(level == levels - 1, over, pltpu.roll(here, levels - 1, 0))
            diagonal = 1.0 - courant - rising - sinking - loss[part, own]
            pieces.append(diagonal * here + total + rising * upper + sinking * lower)
        value = jnp.concatenate(pieces, axis=0).astype(jnp.bfloat16)
        adj[:, out] = value
        if lo == 0:
            adj[:, pl.ds(cols, span)] = value[:, :span]

    for copy in (*halo_parts, *coef_edges):
        copy.wait_recv()
    finish_halo()

    @pl.when(parity == 0)
    def _():
        arrived("g0l", "g7h", "w7", "g5l", "c6")
        finish(0, span, (0, 0), (7, half))
        finish(7 * span, span, (7, 0))
        finish(5 * span, span, (5, 0), (4, half))
        finish(6 * span, span, (6, 0))

    @pl.when(parity == 1)
    def _():
        arrived("g0l", "g7h", "c7", "g6l", "g5w")
        finish(0, span, (0, 0), (7, half))
        finish(7 * span, span, (7, 0))
        finish(5 * span, span, (5, 0), (4, half))
        finish(6 * span, span, (6, 0), (5, half))

    for lo, hi in early:
        tangent_partial(lo, hi)
    level_start(0)

    @pl.when(parity == 0)
    def _():
        arrived("u1", "c2")
        finish(span, span, (1, 0))
        finish(2 * span, span, (2, 0))

    @pl.when(parity == 1)
    def _():
        arrived("c1", "u2")
        finish(span, span, (1, 0))
        finish(2 * span, span, (2, 0))

    for lo, hi in middle:
        tangent_partial(lo, hi)
    level_start(1)

    @pl.when(parity == 0)
    def _():
        arrived("g2h", "g3w")
        finish(3 * span, span, (3, 0), (2, half))
        finish(4 * span, span, (4, 0), (3, half))

    @pl.when(parity == 1)
    def _():
        arrived("g3h", "c3")
        finish(3 * span, span, (3, 0))
        finish(4 * span, span, (4, 0), (3, half))

    for lo, hi in late:
        tangent_partial(lo, hi)
    level_start(2)
    level_wait(0)
    for lo, hi in early:
        tangent_finish(lo, hi)
    for core in BOTH:

        @pl.when(parity == core)
        def _():
            for name, copy in forward.items():
                if core in plan[name][0]:
                    copy.wait_send()

    level_wait(1)
    for lo, hi in middle:
        tangent_finish(lo, hi)
    adjoint(0, 4)
    giving[0].start()
    adjoint(12, tiles)
    for d in (7, 6):
        giving[d].start()
    level_wait(2)
    for lo, hi in late:
        tangent_finish(lo, hi)
    adjoint(4, 6)
    giving[1].start()
    adjoint(6, 12)
    for d in (2, 5, 3):
        giving[d].start()

    def grads(groups):
        for d in groups:
            if d != centre:
                giving[d].wait_recv()
        for d in groups:
            returned = adj[:, pl.ds(d * span, win)] if d == centre else back[d]
            grad = jnp.dot(returned, shifted[d], preferred_element_type=jnp.float32)
            for t in range(parts + 1):
                placed[d, t + 1] = grad[:, t * LANES : (t + 1) * LANES]

    top = placed.shape[1] - 1

    def unslot(groups, again):
        for t in range(tiles):
            value = None
            for d in groups:
                piece = placed[d, lax.min(lax.max(t + 1 - firsts[d], 0), top)]
                value = piece if value is None else value + piece
            for m in range(tracers):
                part = value[m * levels : (m + 1) * levels]
                if again:
                    part = part + grad_out[m, :, pl.ds(t * LANES, LANES)]
                grad_out[m, :, pl.ds(t * LANES, LANES)] = part

    for again, groups in ((False, (centre, 3, 5, 6)), (True, (2, 7)), (True, (1, 0))):
        grads(groups)
        unslot(groups, again)

    for copy in (*giving.values(), *coef_edges, *halo_parts):
        copy.wait_send()

    @pl.when(lev < n_lev - 1)
    def _():
        for copies in level_up:
            for copy in copies:
                copy.wait_send()

    @pl.when(lev > 0)
    def _():
        for copies in level_down:
            for copy in copies:
                copy.wait_send()


def store(tangent_ref, grad_ref, tangent_hbm, grad_hbm, sem):
    copies = [
        pltpu.make_async_copy(tangent_ref, tangent_hbm, sem.at[0]),
        pltpu.make_async_copy(grad_ref, grad_hbm, sem.at[1]),
    ]
    for copy in copies:
        copy.start()
    for copy in copies:
        copy.wait()


def shards(n_tile, n_lev, trajectory, increment, counts, remap_weight, kappa, courant, vertical, offset):
    tracers, levels, cols = trajectory.shape
    reach, win, cap = remap_weight.shape[1:]
    rows = tracers * levels
    span = cols // reach
    wide = cols + 2 * LANES
    f32, bf16 = jnp.float32, jnp.bfloat16
    vmem = pl.BlockSpec(memory_space=pltpu.VMEM)
    dma = pltpu.SemaphoreType.DMA
    out = jax.ShapeDtypeStruct((tracers, levels, cols), f32)
    results = pl.pallas_call(
        functools.partial(kernel, n_tile, n_lev),
        out_shape=(out, out),
        in_specs=[pl.BlockSpec(memory_space=pltpu.HBM)] * 8,
        out_specs=(vmem, vmem),
        scratch_shapes=[
            pltpu.VMEM((tracers, levels, cols), bf16),
            pltpu.VMEM((tracers, levels, cols), bf16),
            pltpu.SMEM((1, reach), jnp.int32),
            pltpu.SMEM((tracers,), f32),
            pltpu.VMEM((1, cols), f32),
            pltpu.VMEM((1, cols), f32),
            pltpu.VMEM((1, cols), jnp.int32),
            pltpu.VMEM((reach, win, cap), bf16),
            pltpu.VMEM((reach, win, cap + LANES), bf16),
            pltpu.VMEM((cols // LANES + cap // LANES + 1, 2 * rows, LANES), bf16),
            pltpu.VMEM((reach, 2 * rows, win), f32),
            pltpu.VMEM((6, 2 * rows, win // 2), f32),
            pltpu.VMEM((5, 2 * rows, win // 2), f32),
            pltpu.VMEM((reach, 2 * rows, win), f32),
            pltpu.VMEM((8, wide), f32),
            pltpu.VMEM((rows, wide + 2 * LANES), f32),
            pltpu.VMEM((rows, wide), f32),
            pltpu.VMEM((rows, wide), f32),
            pltpu.VMEM((8, wide), f32),
            pltpu.VMEM((8, wide), f32),
            pltpu.VMEM((8, wide), f32),
            pltpu.VMEM((8, wide), f32),
            pltpu.VMEM((4, 8, LANES), f32),
            pltpu.VMEM((4, 8, LANES), f32),
            pltpu.VMEM((LANES, LANES), f32),
            pltpu.VMEM((rows, cols + span), bf16),
            pltpu.VMEM((reach, rows, win), bf16),
            pltpu.VMEM((reach, cap // LANES + 3, rows, LANES), f32),
            dma((7,)),
            dma((len(FIRST),)),
            dma((13,)),
            dma((14,)),
            dma((2,)),
            dma((2,)),
            dma((4,)),
            dma((4,)),
            dma((8,)),
            dma((8,)),
            dma((reach,)),
        ],
        compiler_params=pltpu.CompilerParams(
            collective_id=0, has_side_effects=True, vmem_limit_bytes=24 * 1024 * 1024
        ),
    )(
        *(
            pltpu.with_memory_space_constraint(operand, pltpu.HBM)
            for operand in (
                trajectory,
                increment,
                counts,
                kappa,
                courant.reshape(1, cols),
                vertical.reshape(1, cols),
                offset.reshape(1, cols),
                remap_weight,
            )
        )
    )
    return pl.pallas_call(
        store,
        out_shape=(out, out),
        in_specs=(vmem, vmem),
        out_specs=[pl.BlockSpec(memory_space=pltpu.HBM)] * 2,
        scratch_shapes=[dma((2,))],
        compiler_params=pltpu.CompilerParams(vmem_limit_bytes=1024 * 1024),
    )(*results)


def solution(mesh):
    return jax.shard_map(
        functools.partial(shards, mesh.shape["tile"], mesh.shape["lev"]),
        mesh=mesh,
        in_specs=(
            P(None, "lev", "tile"),
            P(None, "lev", "tile"),
            P("tile", None),
            P("tile", None, None, None),
            P(),
            P("tile"),
            P("tile"),
            P("tile"),
        ),
        out_specs=(P(None, "lev", "tile"), P(None, "lev", "tile")),
        check_vma=False,
    )
```

```python
import functools

import jax
import jax.numpy as jnp
from jax import lax
from jax.experimental import pallas as pl
from jax.experimental.pallas import tpu as pltpu
from jax.sharding import PartitionSpec as P

MESH = pl.DeviceIdType.MESH
LANES = 128
HALO = 2
FIRST, SECOND, THIRD = (0,), (7, 6, 1), (2, 3, 5, 4)
REST = SECOND + THIRD
EVEN, ODD = (0,), (1,)
BOTH = (0, 1)


def kernel(
    n_tile,
    n_lev,
    traj_hbm,
    inc_hbm,
    counts_hbm,
    kappa_hbm,
    courant_hbm,
    vertical_hbm,
    offset_hbm,
    weight_hbm,
    tangent_out,
    grad_out,
    traj_ref,
    inc_ref,
    counts_ref,
    kappa_ref,
    courant_ref,
    vertical_ref,
    offset_ref,
    weight,
    shifted,
    fields,
    outgoing,
    mixing,
    summed,
    recv,
    coef,
    delta,
    loss,
    tang,
    up_out,
    down_out,
    below_in,
    above_in,
    tiny_out,
    tiny_in,
    turn,
    adj,
    back,
    placed,
    load_sem,
    weight_sem,
    fwd_send,
    fwd_recv,
    coef_send,
    coef_recv,
    tiny_send,
    tiny_recv,
    lev_send,
    lev_recv,
    ret_recv,
):
    tracers, levels, cols = traj_hbm.shape
    rows = tracers * levels
    reach = weight_hbm.shape[1]
    win, cap = weight_hbm.shape[2], weight_hbm.shape[3]
    centre = reach // 2
    span = cols // reach
    tiles = cols // LANES
    sub = span // LANES
    me = lax.axis_index("tile")
    lev = lax.axis_index("lev")

    def tile_at(distance):
        return (lax.rem(me + (n_tile + distance), n_tile), lev)

    barrier = pltpu.get_barrier_semaphore()
    radius = centre + 1
    for distance in range(-radius, radius + 1):
        if distance != 0:
            pl.semaphore_signal(barrier, inc=1, device_id=tile_at(distance), device_id_type=MESH)

    @pl.when(lev > 0)
    def _():
        pl.semaphore_signal(barrier, inc=1, device_id=(me, lev - 1), device_id_type=MESH)

    @pl.when(lev < n_lev - 1)
    def _():
        pl.semaphore_signal(barrier, inc=1, device_id=(me, lev + 1), device_id_type=MESH)

    loads = [
        pltpu.make_async_copy(source, target, load_sem.at[i])
        for i, (source, target) in enumerate(
            (
                (counts_hbm, counts_ref),
                (kappa_hbm, kappa_ref),
                (traj_hbm, traj_ref),
                (inc_hbm, inc_ref),
                (courant_hbm, courant_ref),
                (vertical_hbm, vertical_ref),
                (offset_hbm, offset_ref),
            )
        )
    ]
    weight_copies = {
        d: pltpu.make_async_copy(weight_hbm.at[0, d], weight.at[d], sem)
        for group, sems in ((FIRST, weight_sem), (REST, load_sem))
        for d, sem in ((d, sems.at[i]) for i, d in enumerate(group))
    }
    for copy in loads:
        copy.start()
    for d in FIRST:
        weight_copies[d].start()

    for copy in loads:
        copy.wait()
    for d in REST:
        weight_copies[d].start()
    stacked = jnp.concatenate(
        [ref[m].astype(jnp.float32) for ref in (traj_ref, inc_ref) for m in range(tracers)], axis=0
    ).astype(jnp.bfloat16)
    for t in range(tiles):
        fields[t] = stacked[:, t * LANES : (t + 1) * LANES]
    for t in range(tiles, fields.shape[0]):
        fields[t] = jnp.zeros((2 * rows, LANES), jnp.bfloat16)
    vertical = vertical_ref[...]
    coef[pl.ds(0, 1), pl.ds(LANES, cols)] = courant_ref[...]
    coef[pl.ds(1, 1), pl.ds(LANES, cols)] = offset_ref[...].astype(jnp.float32)
    coef[pl.ds(2, 1), pl.ds(LANES, cols)] = jnp.maximum(vertical, 0.0)
    coef[pl.ds(3, 1), pl.ds(LANES, cols)] = jnp.maximum(-vertical, 0.0)
    coef[pl.ds(4, 4), pl.ds(LANES, cols)] = jnp.zeros((4, cols), jnp.float32)
    for ref in (up_out, down_out):
        ref[pl.ds(6, 2), :] = jnp.zeros((2, ref.shape[1]), jnp.float32)
    turn[...] = jnp.zeros_like(turn)
    for at in (0, delta.shape[1] - LANES):
        delta[:, pl.ds(at, LANES)] = jnp.zeros((rows, LANES), jnp.float32)

    @pl.when(lev == 0)
    def _():
        below_in[...] = jnp.zeros_like(below_in)

    @pl.when(lev == n_lev - 1)
    def _():
        above_in[...] = jnp.zeros_like(above_in)

    placed[:, pl.ds(0, 1)] = jnp.zeros((reach, 1, rows, LANES), jnp.float32)
    placed[:, pl.ds(placed.shape[1] - 1, 1)] = jnp.zeros((reach, 1, rows, LANES), jnp.float32)

    starts = []
    total = jnp.int32(0)
    for d in range(reach):
        starts.append(total)
        total = total + counts_ref[0, d]

    firsts = [lax.shift_right_logical(start, 7) for start in starts]
    shifts = [lax.bitwise_and(start, LANES - 1) for start in starts]
    parts = cap // LANES
    lane = lax.broadcasted_iota(jnp.int32, (2 * rows, LANES), 1)
    skew = lax.broadcasted_iota(jnp.int32, (2 * LANES, LANES), 0) - lax.broadcasted_iota(
        jnp.int32, (2 * LANES, LANES), 1
    )

    def selection(amount):
        return jnp.where(skew == amount, 1.0, 0.0).astype(jnp.bfloat16)

    def slots_of(d):
        loaded = [fields[firsts[d] + t] for t in range(parts + 1)]
        pairs = [jnp.concatenate([loaded[t], loaded[t + 1]], axis=1) for t in range(parts)]
        moved = jnp.dot(
            jnp.concatenate(pairs, axis=0), selection(shifts[d]), preferred_element_type=jnp.float32
        )
        pieces = []
        for t in range(parts):
            value = moved[t * 2 * rows : (t + 1) * 2 * rows]
            pieces.append(jnp.where(lane + t * LANES < counts_ref[0, d], value, 0.0).astype(jnp.bfloat16))
        return jnp.concatenate(pieces, axis=1)

    tall = lax.broadcasted_iota(jnp.int32, (win, LANES), 1)

    def place_weight(d):
        chosen = selection(LANES - shifts[d])
        nothing = jnp.zeros((win, LANES), jnp.bfloat16)
        live = []
        for t in range(parts):
            piece = weight[d, :, pl.ds(t * LANES, LANES)]
            live.append(jnp.where(tall + t * LANES < counts_ref[0, d], piece, nothing))
        live = [nothing, *live, nothing]
        for t in range(parts + 1):
            moved = jnp.dot(
                jnp.concatenate([live[t], live[t + 1]], axis=1), chosen, preferred_element_type=jnp.float32
            )
            shifted[d, :, pl.ds(t * LANES, LANES)] = moved.astype(jnp.bfloat16)

    parity = lax.rem(me, 2)
    half = win // 2

    def on_core(cores, run):
        if len(cores) == 2:
            run()
        else:
            pl.when(parity == cores[0])(run)

    def window_part(d, lane, width):
        part = pl.ds(lane, width)
        return outgoing.at[d, :, part], recv.at[d, :, part], d - centre

    plan = {
        "g0l": (BOTH, 0, 0, *window_part(0, 0, half)),
        "g2h": (EVEN, 2, 2, *window_part(2, half, half)),
        "g3h": (EVEN, 3, 3, *window_part(3, half, half)),
        "g3w": (ODD, 3, 3, *window_part(3, 0, win)),
        "g5w": (EVEN, 4, 4, *window_part(5, 0, win)),
        "g5l": (ODD, 4, 4, *window_part(5, 0, half)),
        "g6l": (ODD, 5, 5, *window_part(6, 0, half)),
        "g7h": (BOTH, 6, 6, *window_part(7, half, half)),
        "m1": (EVEN, 7, 10, outgoing.at[1, :, pl.ds(0, half)], mixing.at[0], 1),
        "m2": (EVEN, 8, 11, outgoing.at[2, :, pl.ds(0, half)], mixing.at[1], 1),
        "m3": (EVEN, 9, 12, outgoing.at[3, :, pl.ds(0, half)], mixing.at[2], 1),
        "m5": (ODD, 7, 10, outgoing.at[5, :, pl.ds(half, half)], mixing.at[0], -1),
        "m6": (ODD, 8, 11, outgoing.at[6, :, pl.ds(half, half)], mixing.at[1], -1),
        "v7": (ODD, 12, 12, outgoing.at[7, :, pl.ds(0, half)], mixing.at[5], 1),
        "t0": (EVEN, 1, 1, outgoing.at[0, :, pl.ds(half, half)], mixing.at[3], -1),
        "t1": (EVEN, 12, 13, outgoing.at[1, :, pl.ds(half, half)], mixing.at[4], -1),
        "u1": (ODD, 1, 1, summed.at[3], recv.at[1, :, pl.ds(0, half)], -3),
        "u2": (ODD, 2, 2, summed.at[4], recv.at[2, :, pl.ds(0, half)], -2),
        "c1": (ODD, 9, 7, summed.at[0], recv.at[1, :, pl.ds(0, half)], -4),
        "c2": (ODD, 10, 7, summed.at[1], recv.at[2, :, pl.ds(0, half)], -3),
        "c3": (ODD, 11, 8, summed.at[2], recv.at[3, :, pl.ds(0, half)], -2),
        "w7": (EVEN, 5, 5, summed.at[2], recv.at[7, :, pl.ds(0, half)], 2),
        "c6": (EVEN, 10, 8, summed.at[0], recv.at[6, :, pl.ds(0, half)], 2),
        "c7": (EVEN, 11, 9, summed.at[1], recv.at[7, :, pl.ds(0, half)], 3),
    }
    forward = {
        name: pltpu.make_async_remote_copy(
            src_ref=source,
            dst_ref=target,
            send_sem=fwd_send,
            recv_sem=fwd_recv.at[landing],
            device_id=tile_at(distance),
            device_id_type=MESH,
        )
        for name, (_, _, landing, source, target, distance) in plan.items()
    }
    corners = ((0, 0, 0, -5), (7, half, 0, 2), (7, half - 16, 8, 4), (6, win - 16, 8, 3))
    halo_parts = [
        pltpu.make_async_remote_copy(
            src_ref=tiny_out.at[i],
            dst_ref=tiny_in.at[i],
            send_sem=tiny_send,
            recv_sem=tiny_recv,
            device_id=tile_at(distance),
            device_id_type=MESH,
        )
        for i, (_, _, _, distance) in enumerate(corners)
    ]

    def send(*names):
        for name in names:
            on_core(plan[name][0], forward[name].start)

    def arrived(*names):
        for name in names:
            forward[name].wait_recv()

    giving = {
        d: pltpu.make_async_remote_copy(
            src_ref=adj.at[:, pl.ds(d * span, win)],
            dst_ref=back.at[d],
            send_sem=fwd_send,
            recv_sem=ret_recv.at[d],
            device_id=tile_at(centre - d),
            device_id_type=MESH,
        )
        for d in range(reach)
        if d != centre
    }

    coef_edges = [
        pltpu.make_async_remote_copy(
            src_ref=coef.at[:, pl.ds(source, LANES)],
            dst_ref=coef.at[:, pl.ds(target, LANES)],
            send_sem=coef_send.at[i],
            recv_sem=coef_recv.at[i],
            device_id=tile_at(distance),
            device_id_type=MESH,
        )
        for i, (source, target, distance) in enumerate(((LANES, LANES + cols, -1), (cols, 0, 1)))
    ]

    early = ((-1, 1), (11, tiles + 1))
    middle = ((1, 5),)
    late = ((5, 11),)
    level_up, level_down = ([], [], []), ([], [], [])
    index = 0
    for stage, ranges in enumerate((early, middle, late)):
        for lo, hi in ranges:
            part = pl.ds((lo + 1) * LANES, (hi - lo) * LANES)
            for ways, source, target, distance, sent in (
                (level_up, up_out, below_in, 1, lev_send.at[0]),
                (level_down, down_out, above_in, n_lev - 1, lev_send.at[1]),
            ):
                ways[stage].append(
                    pltpu.make_async_remote_copy(
                        src_ref=source.at[:, part],
                        dst_ref=target.at[:, part],
                        send_sem=sent,
                        recv_sem=lev_recv.at[index],
                        device_id=(me, lax.rem(lev + distance, n_lev)),
                        device_id_type=MESH,
                    )
                )
                index += 1

    def all_of(source, target, send_sem, recv_sem):
        return pltpu.make_async_remote_copy(
            src_ref=source,
            dst_ref=target,
            send_sem=send_sem,
            recv_sem=recv_sem,
            device_id=tile_at(1),
            device_id_type=MESH,
        )

    seven = pl.ds(0, reach - 1)
    all_forward = all_of(outgoing.at[seven], outgoing.at[seven], fwd_send, fwd_recv.at[0])
    all_returns = all_of(back.at[seven], back.at[seven], fwd_send, fwd_recv.at[0])
    all_halo = all_of(tiny_out, tiny_in, tiny_send, tiny_recv)
    all_up = all_of(up_out, below_in, lev_send.at[0], lev_recv.at[0])
    all_down = all_of(down_out, above_in, lev_send.at[1], lev_recv.at[0])

    def level_start(stage):
        @pl.when(lev < n_lev - 1)
        def _():
            for copy in level_up[stage]:
                copy.start()

        @pl.when(lev > 0)
        def _():
            for copy in level_down[stage]:
                copy.start()

    def level_wait(stage):
        @pl.when(lev > 0)
        def _():
            for copy in level_up[stage]:
                copy.wait_recv()

        @pl.when(lev < n_lev - 1)
        def _():
            for copy in level_down[stage]:
                copy.wait_recv()

    sends = {
        0: ("t0", "g0l"),
        7: ("v7", "g7h"),
        6: ("m6", "g6l"),
        1: ("m1", "t1"),
        2: ("m2", "g2h"),
        3: ("m3", "g3h", "g3w"),
        5: ("m5", "g5w", "g5l"),
    }

    def windows(groups):
        slotted = {d: slots_of(d) for d in groups}
        for d in groups:
            weight_copies[d].wait()
        for i, (d, column, row, _) in enumerate(corners):
            if d in groups:
                corner = lax.dot_general(
                    weight[d, pl.ds(column, 16), :],
                    slotted[d],
                    (((1,), (1,)), ((), ())),
                    preferred_element_type=jnp.float32,
                )
                tiny_out[i, :, pl.ds(0, 2 * rows)] = corner[row : row + 8]
        for d in groups:
            window = lax.dot_general(
                slotted[d], weight[d], (((1,), (1,)), ((), ())), preferred_element_type=jnp.float32
            )
            if d == centre:
                recv[d] = window
            else:
                outgoing[d] = window

    tiny_out[...] = jnp.zeros_like(tiny_out)
    windows(FIRST)
    pl.semaphore_wait(
        barrier, 2 * radius + (lev > 0).astype(jnp.int32) + (lev < n_lev - 1).astype(jnp.int32)
    )
    for copy in coef_edges:
        copy.start()

    def send_group(group):
        for copy, corner in zip(halo_parts, corners):
            if corner[0] in group:
                copy.start()
        for d in group:
            if d != centre:
                send(*sends[d])

    send_group(FIRST)
    for group in (SECOND, THIRD):
        windows(group)
        send_group(group)
    def add(name, slot, d, at, sum_name, mixed):
        forward[name].wait_recv()
        summed[slot] = outgoing[d, :, pl.ds(at, half)] + mixing[mixed]
        forward[sum_name].start()

    for d in (7, 6, 1):
        place_weight(d)

    @pl.when(parity == 1)
    def _():
        add("m1", 0, 0, half, "c1", 0)
        add("m2", 1, 1, half, "c2", 1)
        add("m3", 2, 2, half, "c3", 2)

    @pl.when(parity == 0)
    def _():
        add("m6", 1, 7, 0, "c7", 1)
        add("v7", 2, 6, half, "w7", 5)
        add("m5", 0, 6, 0, "c6", 0)

    for d in (0, 2):
        place_weight(d)

    @pl.when(parity == 1)
    def _():
        add("t0", 3, 1, 0, "u1", 3)

    for d in (3, 5):
        place_weight(d)

    @pl.when(parity == 1)
    def _():
        add("t1", 4, 2, 0, "u2", 4)

    place_weight(centre)

    def finish(column, width, *pieces):
        value = None
        for d, at in pieces:
            piece = recv[d, :, pl.ds(at, width)]
            value = piece if value is None else value + piece
        for m in range(tracers):
            part = pl.ds(m * levels, levels)
            loss[part, pl.ds(LANES + column, width)] = 2.0 * kappa_ref[m] * value[m * levels : (m + 1) * levels]
        delta[:, pl.ds(2 * LANES + column, width)] = value[rows:]

    def finish_halo():
        turn[pl.ds(0, 8), :] = tiny_in[0] + tiny_in[1]
        turn[pl.ds(LANES - 8, 8), :] = tiny_in[2] + tiny_in[3]
        value = jnp.transpose(turn[...])
        for at in (0, LANES + cols):
            for m in range(tracers):
                part = pl.ds(m * levels, levels)
                loss[part, pl.ds(at, LANES)] = 2.0 * kappa_ref[m] * value[m * levels : (m + 1) * levels]
            delta[:, pl.ds(LANES + at, LANES)] = value[rows : 2 * rows]

    def level_rows(width):
        return lax.broadcasted_iota(jnp.int32, (levels, width), 0)

    def tangent_partial(lo, hi):
        width = (hi - lo) * LANES
        own = pl.ds(LANES + lo * LANES, width)
        courant, offset = coef[pl.ds(0, 1), own], coef[pl.ds(1, 1), own]
        rising, sinking = coef[pl.ds(2, 1), own], coef[pl.ds(3, 1), own]
        level = level_rows(width)
        for m in range(tracers):
            part = pl.ds(m * levels, levels)
            wide = delta[part, pl.ds((lo + 1) * LANES, width + 2 * LANES)]
            here = wide[:, LANES : LANES + width]
            departed = jnp.zeros_like(here)
            for shift in range(-HALO, HALO + 1):
                moved = here
                if shift != 0:
                    moved = pltpu.roll(wide, (-shift) % (width + 2 * LANES), 1)[:, LANES : LANES + width]
                departed = jnp.where(offset == float(shift), moved, departed)
            below = jnp.where(level == 0, 0.0, pltpu.roll(here, 1, 0))
            above = jnp.where(level == levels - 1, 0.0, pltpu.roll(here, levels - 1, 0))
            value = (
                here
                + courant * (departed - here)
                + rising * (below - here)
                + sinking * (above - here)
                - loss[part, own] * here
            )
            tang[part, own] = value
            up_out[pl.ds(m, 1), own] = value[levels - 1 : levels]
            up_out[pl.ds(tracers + m, 1), own] = here[levels - 1 : levels]
            down_out[pl.ds(m, 1), own] = value[0:1]
            down_out[pl.ds(tracers + m, 1), own] = here[0:1]

    def tangent_finish(lo, hi):
        width = (hi - lo) * LANES
        own = pl.ds(LANES + lo * LANES, width)
        rising, sinking = coef[pl.ds(2, 1), own], coef[pl.ds(3, 1), own]
        level = level_rows(width)
        inner_lo, inner_hi = max(lo, 0), min(hi, tiles)
        for m in range(tracers):
            part = pl.ds(m * levels, levels)
            value = tang[part, own]
            value = value + jnp.where(level == 0, rising * below_in[pl.ds(tracers + m, 1), own], 0.0)
            value = value + jnp.where(level == levels - 1, sinking * above_in[pl.ds(tracers + m, 1), own], 0.0)
            tang[part, own] = value
            tangent_out[m, :, pl.ds(inner_lo * LANES, (inner_hi - inner_lo) * LANES)] = value[
                :, (inner_lo - lo) * LANES : (inner_hi - lo) * LANES
            ]

    def adjoint(lo, hi):
        width = (hi - lo) * LANES
        own = pl.ds(LANES + lo * LANES, width)
        out = pl.ds(lo * LANES, width)
        around = pl.ds(lo * LANES, width + 2 * LANES)
        courant, rising, sinking = coef[pl.ds(0, 1), own], coef[pl.ds(2, 1), own], coef[pl.ds(3, 1), own]
        wide_courant, wide_offset = coef[pl.ds(0, 1), around], coef[pl.ds(1, 1), around]
        level = level_rows(width)
        pieces = []
        for m in range(tracers):
            part = pl.ds(m * levels, levels)
            wide = tang[part, around]
            here = wide[:, LANES : LANES + width]
            total = jnp.zeros_like(here)
            for shift in range(-HALO, HALO + 1):
                term = jnp.where(wide_offset == float(shift), wide_courant, 0.0) * wide
                if shift != 0:
                    term = pltpu.roll(term, shift % (width + 2 * LANES), 1)
                total = total + term[:, LANES : LANES + width]
            own_delta = delta[part, pl.ds((lo + 2) * LANES, width)]
            under = below_in[pl.ds(m, 1), own] + sinking * own_delta[0:1]
            over = above_in[pl.ds(m, 1), own] + rising * own_delta[levels - 1 : levels]
            under = jnp.where(lev > 0, under, 0.0)
            over = jnp.where(lev < n_lev - 1, over, 0.0)
            lower = jnp.where(level == 0, under, pltpu.roll(here, 1, 0))
            upper = jnp.where(level == levels - 1, over, pltpu.roll(here, levels - 1, 0))
            diagonal = 1.0 - courant - rising - sinking - loss[part, own]
            pieces.append(diagonal * here + total + rising * upper + sinking * lower)
        value = jnp.concatenate(pieces, axis=0).astype(jnp.bfloat16)
        adj[:, out] = value
        if lo == 0:
            adj[:, pl.ds(cols, span)] = value[:, :span]

    for copy in (all_halo, *coef_edges):
        copy.wait_recv()
    finish_halo()

    @pl.when(parity == 0)
    def _():
        arrived("g0l", "g7h", "w7", "g5l", "c6")
        finish(0, span, (0, 0), (7, half))
        finish(7 * span, span, (7, 0))
        finish(5 * span, span, (5, 0), (4, half))
        finish(6 * span, span, (6, 0))

    @pl.when(parity == 1)
    def _():
        arrived("g0l", "g7h", "c7", "g6l", "g5w")
        finish(0, span, (0, 0), (7, half))
        finish(7 * span, span, (7, 0))
        finish(5 * span, span, (5, 0), (4, half))
        finish(6 * span, span, (6, 0), (5, half))

    for lo, hi in early:
        tangent_partial(lo, hi)
    level_start(0)

    @pl.when(parity == 0)
    def _():
        arrived("u1", "c2")
        finish(span, span, (1, 0))
        finish(2 * span, span, (2, 0))

    @pl.when(parity == 1)
    def _():
        arrived("c1", "u2")
        finish(span, span, (1, 0))
        finish(2 * span, span, (2, 0))

    for lo, hi in middle:
        tangent_partial(lo, hi)
    level_start(1)

    @pl.when(parity == 0)
    def _():
        arrived("g2h", "g3w")
        finish(3 * span, span, (3, 0), (2, half))
        finish(4 * span, span, (4, 0), (3, half))

    @pl.when(parity == 1)
    def _():
        arrived("g3h", "c3")
        finish(3 * span, span, (3, 0))
        finish(4 * span, span, (4, 0), (3, half))

    for lo, hi in late:
        tangent_partial(lo, hi)
    level_start(2)
    level_wait(0)
    for lo, hi in early:
        tangent_finish(lo, hi)
    all_forward.wait_send()
    level_wait(1)
    for lo, hi in middle:
        tangent_finish(lo, hi)
    adjoint(0, 4)
    giving[0].start()
    adjoint(12, tiles)
    for d in (7, 6):
        giving[d].start()
    level_wait(2)
    for lo, hi in late:
        tangent_finish(lo, hi)
    adjoint(4, 6)
    giving[1].start()
    adjoint(6, 12)
    for d in (2, 5, 3):
        giving[d].start()

    def grads(groups):
        for d in groups:
            if d != centre:
                giving[d].wait_recv()
        for d in groups:
            returned = adj[:, pl.ds(d * span, win)] if d == centre else back[d]
            grad = jnp.dot(returned, shifted[d], preferred_element_type=jnp.float32)
            for t in range(parts + 1):
                placed[d, t + 1] = grad[:, t * LANES : (t + 1) * LANES]

    top = placed.shape[1] - 1

    def unslot(groups, again):
        for t in range(tiles):
            value = None
            for d in groups:
                piece = placed[d, lax.min(lax.max(t + 1 - firsts[d], 0), top)]
                value = piece if value is None else value + piece
            for m in range(tracers):
                part = value[m * levels : (m + 1) * levels]
                if again:
                    part = part + grad_out[m, :, pl.ds(t * LANES, LANES)]
                grad_out[m, :, pl.ds(t * LANES, LANES)] = part

    for again, groups in ((False, (centre, 3, 5, 6)), (True, (2, 7)), (True, (1, 0))):
        grads(groups)
        unslot(groups, again)

    for copy in (all_returns, all_halo, *coef_edges):
        copy.wait_send()

    @pl.when(lev < n_lev - 1)
    def _():
        all_up.wait_send()

    @pl.when(lev > 0)
    def _():
        all_down.wait_send()


def store(tangent_ref, grad_ref, tangent_hbm, grad_hbm, sem):
    copies = [
        pltpu.make_async_copy(tangent_ref, tangent_hbm, sem.at[0]),
        pltpu.make_async_copy(grad_ref, grad_hbm, sem.at[1]),
    ]
    for copy in copies:
        copy.start()
    for copy in copies:
        copy.wait()


def shards(n_tile, n_lev, trajectory, increment, counts, remap_weight, kappa, courant, vertical, offset):
    tracers, levels, cols = trajectory.shape
    reach, win, cap = remap_weight.shape[1:]
    rows = tracers * levels
    span = cols // reach
    wide = cols + 2 * LANES
    f32, bf16 = jnp.float32, jnp.bfloat16
    vmem = pl.BlockSpec(memory_space=pltpu.VMEM)
    dma = pltpu.SemaphoreType.DMA
    out = jax.ShapeDtypeStruct((tracers, levels, cols), f32)
    results = pl.pallas_call(
        functools.partial(kernel, n_tile, n_lev),
        out_shape=(out, out),
        in_specs=[pl.BlockSpec(memory_space=pltpu.HBM)] * 8,
        out_specs=(vmem, vmem),
        scratch_shapes=[
            pltpu.VMEM((tracers, levels, cols), bf16),
            pltpu.VMEM((tracers, levels, cols), bf16),
            pltpu.SMEM((1, reach), jnp.int32),
            pltpu.SMEM((tracers,), f32),
            pltpu.VMEM((1, cols), f32),
            pltpu.VMEM((1, cols), f32),
            pltpu.VMEM((1, cols), jnp.int32),
            pltpu.VMEM((reach, win, cap), bf16),
            pltpu.VMEM((reach, win, cap + LANES), bf16),
            pltpu.VMEM((cols // LANES + cap // LANES + 1, 2 * rows, LANES), bf16),
            pltpu.VMEM((reach, 2 * rows, win), f32),
            pltpu.VMEM((6, 2 * rows, win // 2), f32),
            pltpu.VMEM((5, 2 * rows, win // 2), f32),
            pltpu.VMEM((reach, 2 * rows, win), f32),
            pltpu.VMEM((8, wide), f32),
            pltpu.VMEM((rows, wide + 2 * LANES), f32),
            pltpu.VMEM((rows, wide), f32),
            pltpu.VMEM((rows, wide), f32),
            pltpu.VMEM((8, wide), f32),
            pltpu.VMEM((8, wide), f32),
            pltpu.VMEM((8, wide), f32),
            pltpu.VMEM((8, wide), f32),
            pltpu.VMEM((4, 8, LANES), f32),
            pltpu.VMEM((4, 8, LANES), f32),
            pltpu.VMEM((LANES, LANES), f32),
            pltpu.VMEM((rows, cols + span), bf16),
            pltpu.VMEM((reach, rows, win), bf16),
            pltpu.VMEM((reach, cap // LANES + 3, rows, LANES), f32),
            dma((7,)),
            dma((len(FIRST),)),
            dma,
            dma((14,)),
            dma((2,)),
            dma((2,)),
            dma,
            dma,
            dma((2,)),
            dma((8,)),
            dma((reach,)),
        ],
        compiler_params=pltpu.CompilerParams(
            collective_id=0, has_side_effects=True, vmem_limit_bytes=24 * 1024 * 1024
        ),
    )(
        *(
            pltpu.with_memory_space_constraint(operand, pltpu.HBM)
            for operand in (
                trajectory,
                increment,
                counts,
                kappa,
                courant.reshape(1, cols),
                vertical.reshape(1, cols),
                offset.reshape(1, cols),
                remap_weight,
            )
        )
    )
    return pl.pallas_call(
        store,
        out_shape=(out, out),
        in_specs=(vmem, vmem),
        out_specs=[pl.BlockSpec(memory_space=pltpu.HBM)] * 2,
        scratch_shapes=[dma((2,))],
        compiler_params=pltpu.CompilerParams(vmem_limit_bytes=1024 * 1024),
    )(*results)


def solution(mesh):
    return jax.shard_map(
        functools.partial(shards, mesh.shape["tile"], mesh.shape["lev"]),
        mesh=mesh,
        in_specs=(
            P(None, "lev", "tile"),
            P(None, "lev", "tile"),
            P("tile", None),
            P("tile", None, None, None),
            P(),
            P("tile"),
            P("tile"),
            P("tile"),
        ),
        out_specs=(P(None, "lev", "tile"), P(None, "lev", "tile")),
        check_vma=False,
    )
```
